512 devices in a mesh: groups: 2 (over y), pair: 32 (over z), vir: 4 (over x), sub: 2 (over core).
Axes of the slice: x: 4, y: 2, z: 32, core: 2. Of those that a mesh axis runs over, the one named last changes fastest.
The devices are a block of a 4x8x32 slice.
Arguments:
- amplitudes: bfloat16 [64, 36, 128, 128], P(('groups', 'pair'), 'vir', 'sub'), parts along dimension 0, may hold values from -1 to 1
- pair_list: int32 [64, 2], P(('groups', 'pair')), parts along dimension 0, may hold values from 0 to 255, as said below
- tile_list: int32 [36, 2], replicated, may hold values from 0 to 7, as said below
Outputs:
- p_virt: float32 [72, 128, 128], P(('groups', 'vir'), 'sub'), parts along dimension 0
- p_occ: float32 [512, 256], P('groups'), parts along dimension 0
The draws below stay inside these ranges and needn't reach their ends.
There are 2 independent parts, one for each index of `groups`. The reference program is written for one: setup_inputs(seed, part) draws one part's arguments, and reference() takes and returns one part's arrays. A program takes and returns all parts, laid end to end along the dimension named above; an argument that names none is the same for every part. Nothing has to cross between parts.
Inputs may be any that keep to these rules, and one draw needn't show every extreme that they name: `pair_list`: each row holds two different occupied orbitals in increasing order; no two rows are equal. `tile_list`: each row holds a tile row and a tile column, row <= column; every such couple of the 8 x 8 tile grid appears exactly once.
All inputs are finite; a program needn't handle non-finite values.
Results may differ from the reference program's by a relative error of at most 0.0003.
Values may be sent and summed in bfloat16 or wider, within the bound.
No kernel may reach another device: no remote copies, remote signals or barrier semaphores. Data moves between devices by JAX's collectives and lax.ppermute only.
A program may use at most 64 MiB of HBM per device.

```python
import math
import jax
import jax.numpy as jnp
import numpy as np
from jax import lax

V = 1024
OCC = 256
TILE = 128
NTV = 8
NT = 36
NP = 32


mode_count = 4


def pair_table(key):
    window_width = min(OCC, NP // 4 + 16)
    first_np, second_np = np.triu_indices(window_width, 1)
    chosen = jax.random.permutation(jax.random.fold_in(key, 3), first_np.shape[0])[:NP]
    orbitals = jax.random.permutation(jax.random.fold_in(key, 5), OCC)[:window_width]
    first_name = orbitals[jnp.asarray(first_np, jnp.int32)[chosen]]
    second_name = orbitals[jnp.asarray(second_np, jnp.int32)[chosen]]
    return jnp.stack([jnp.minimum(first_name, second_name), jnp.maximum(first_name, second_name)], axis=1).astype(jnp.int32)


def draw_pair_list(key, part):
    return pair_table(jax.random.fold_in(key, 11))


def draw_tile_list(key, part):
    rows_np, cols_np = np.triu_indices(NTV)
    shuffled = jax.random.permutation(jax.random.fold_in(key, 7), NT)
    tile_rows = jnp.asarray(rows_np, jnp.int32)[shuffled]
    tile_cols = jnp.asarray(cols_np, jnp.int32)[shuffled]
    return jnp.stack([tile_rows, tile_cols], axis=1).astype(jnp.int32)


def draw_amplitudes(key, part):
    pair_rows = pair_table(jax.random.fold_in(key, 11))
    mixing = jax.random.normal(jax.random.fold_in(key, 13), (OCC, mode_count), jnp.float32)
    shapes_common = jax.random.normal(jax.random.fold_in(key, 17), (mode_count, NT, TILE, TILE), jnp.float32)
    own_part = jnp.clip(jax.random.normal(jax.random.fold_in(key, 19), (NP, NT, TILE, TILE), jnp.float32), -6.0, 6.0)
    shared_weight = 0.2
    mixture = mixing[pair_rows[:, 0]] + mixing[pair_rows[:, 1]]
    shared_part = jnp.einsum('pm,mstu->pstu', mixture, shapes_common)
    overall = 1.0 / math.sqrt(2.6 * V * math.sqrt(NP * V))
    return jnp.clip(overall * (own_part + shared_weight * shared_part), -1.0, 1.0).astype(jnp.bfloat16)


def setup_inputs(seed: int = 0, part: int = 0) -> dict:
    arg_keys = jax.random.split(jax.random.key(seed), 4)
    part_keys = jax.random.split(jax.random.fold_in(arg_keys[3], part), 4)
    amplitudes = draw_amplitudes(jax.random.fold_in(jax.random.fold_in(arg_keys[3], part), 71), part)
    pair_list = draw_pair_list(jax.random.fold_in(jax.random.fold_in(arg_keys[3], part), 71), part)
    tile_list = draw_tile_list(jax.random.fold_in(arg_keys[3], 71), part)
    return {"amplitudes": amplitudes, "pair_list": pair_list, "tile_list": tile_list}


def slot_table(tile_list):
    tile_grid = jnp.arange(NTV, dtype=jnp.int32)
    upper_hit = (tile_list[:, 0][None, None, :] == tile_grid[:, None, None]) & (tile_list[:, 1][None, None, :] == tile_grid[None, :, None])
    either_hit = upper_hit | jnp.transpose(upper_hit, (1, 0, 2))
    slot_ids = jnp.arange(NT, dtype=jnp.int32)
    return jnp.sum(jnp.where(either_hit, slot_ids[None, None, :], 0), axis=2).astype(jnp.int32)


def keep_upper(tile_list):
    on_diagonal = tile_list[:, 0] == tile_list[:, 1]
    in_tile = jnp.arange(TILE, dtype=jnp.int32)
    lower_part = in_tile[None, :] <= in_tile[:, None]
    return jnp.logical_not(on_diagonal[:, None, None] & lower_part[None])


def unpack(packed, slot_grid):
    gathered = packed[slot_grid]
    turned = jnp.swapaxes(gathered, 2, 3)
    tile_grid = jnp.arange(NTV, dtype=jnp.int32)
    on_or_above = (tile_grid[:, None] <= tile_grid[None, :])[:, :, None, None]
    on_or_below = (tile_grid[:, None] >= tile_grid[None, :])[:, :, None, None]
    nothing = jnp.zeros_like(gathered)
    whole = jnp.where(on_or_above, gathered, nothing) - jnp.where(on_or_below, turned, nothing)
    return jnp.transpose(whole, (0, 2, 1, 3)).reshape(V, V)


def occurrences(pair_rows):
    orbital = jnp.concatenate([pair_rows[:, 0], pair_rows[:, 1]])
    partner = jnp.concatenate([pair_rows[:, 1], pair_rows[:, 0]])
    pair_count = pair_rows.shape[0]
    parity = jnp.concatenate([jnp.ones((pair_count,), jnp.float32), -jnp.ones((pair_count,), jnp.float32)])
    return orbital, partner, parity


def occ_density(pair_gram, left_pairs, right_pairs):
    left_orb, left_partner, left_sign = occurrences(left_pairs)
    right_orb, right_partner, right_sign = occurrences(right_pairs)
    doubled = jnp.tile(pair_gram, (2, 2))
    couple = jnp.where(left_partner[:, None] == right_partner[None, :], left_sign[:, None] * right_sign[None, :] * doubled, 0.0)
    orbitals = jnp.arange(OCC, dtype=jnp.int32)
    left_hot = (left_orb[:, None] == orbitals[None, :]).astype(jnp.float32)
    right_hot = (right_orb[:, None] == orbitals[None, :]).astype(jnp.float32)
    inner_sum = jnp.dot(couple, right_hot, precision=lax.Precision.HIGHEST)
    return -jnp.dot(left_hot.T, inner_sum, precision=lax.Precision.HIGHEST)


def reference(amplitudes, pair_list, tile_list):
    keep_mask = keep_upper(tile_list)
    masked = jnp.where(keep_mask[None], amplitudes, jnp.zeros((), jnp.bfloat16))
    slot_grid = slot_table(tile_list)

    def add_pair(running, packed):
        whole = unpack(packed, slot_grid)
        return running + jnp.dot(whole, whole.T, preferred_element_type=jnp.float32), None

    density, _ = lax.scan(add_pair, jnp.zeros((V, V), jnp.float32), masked)
    tile_view = jnp.transpose(density.reshape(NTV, TILE, NTV, TILE), (0, 2, 1, 3))
    p_virt = tile_view[tile_list[:, 0], tile_list[:, 1]]
    flat_masked = masked.reshape(NP, NT * TILE * TILE)
    flat_all = amplitudes.reshape(NP, NT * TILE * TILE)
    pair_gram = lax.dot_general(flat_masked, flat_all, (((1,), (1,)), ((), ())), preferred_element_type=jnp.float32)
    p_occ = occ_density(pair_gram, pair_list, pair_list)
    return (p_virt, p_occ)
```

```python
import functools

import jax
import jax.numpy as jnp
from jax import lax
from jax.experimental import pallas as pl
from jax.experimental.pallas import tpu as pltpu
from jax.sharding import Mesh
from jax.sharding import PartitionSpec as P

OCC = 256
NTV = 8
NEAR = 8


def sent_to_all(array, axis):
    copies = jnp.broadcast_to(array, (lax.axis_size(axis), *array.shape))
    return lax.all_to_all(copies, axis, split_axis=0, concat_axis=0, tiled=True)


def occurrences(pair_rows):
    orbital = jnp.concatenate([pair_rows[:, 0], pair_rows[:, 1]])
    partner = jnp.concatenate([pair_rows[:, 1], pair_rows[:, 0]])
    pair_count = pair_rows.shape[0]
    parity = jnp.concatenate(
        [jnp.ones((pair_count,), jnp.float32), -jnp.ones((pair_count,), jnp.float32)]
    )
    return (orbital, partner, parity)


def occ_density(pair_gram, pairs):
    orb, partner, sign = occurrences(pairs)
    doubled = jnp.tile(pair_gram, (2, 2))
    couple = jnp.where(
        partner[:, None] == partner[None, :], sign[:, None] * sign[None, :] * doubled, 0.0
    )
    orbitals = jnp.arange(OCC, dtype=jnp.int32)
    hot = (orb[:, None] == orbitals[None, :]).astype(jnp.float32)
    inner_sum = jnp.dot(couple, hot, precision=lax.Precision.HIGHEST)
    return -jnp.dot(hot.T, inner_sum, precision=lax.Precision.HIGHEST)


def virt_kernel(tiles_ref, place_ref, packed_ref, out_ref, whole_ref, slot_ref):
    slot_count, width, _ = packed_ref.shape
    own_count, own_rows, _ = out_ref.shape

    def note(s, carry):
        slot_ref[tiles_ref[s, 0] * NTV + tiles_ref[s, 1]] = s
        return carry

    lax.fori_loop(0, slot_count, note, 0)
    for r in range(NTV):
        for c in range(r, NTV):
            tile = packed_ref[slot_ref[r * NTV + c]]
            turned = tile.T
            if r == c:
                whole_ref[r, :, c * width : (c + 1) * width] = tile - turned
            else:
                whole_ref[r, :, c * width : (c + 1) * width] = tile
                whole_ref[c, :, r * width : (r + 1) * width] = -turned
    first = place_ref[0]
    half = place_ref[1]
    for i in range(own_count):
        left = whole_ref[tiles_ref[first + i, 0], pl.ds(half * own_rows, own_rows), :]
        right = whole_ref[tiles_ref[first + i, 1]]
        out_ref[i] = lax.dot_general(
            left, right, (((1,), (1,)), ((), ())), preferred_element_type=jnp.float32
        )


def virt_partial(tile_list, place, packed, own_count, own_rows):
    width = packed.shape[2]
    smem = pl.BlockSpec(memory_space=pltpu.SMEM)
    vmem = pl.BlockSpec(memory_space=pltpu.VMEM)
    return pl.pallas_call(
        virt_kernel,
        out_shape=jax.ShapeDtypeStruct((own_count, own_rows, width), jnp.float32),
        in_specs=[smem, smem, vmem],
        out_specs=vmem,
        scratch_shapes=[
            pltpu.VMEM((NTV, width, NTV * width), jnp.bfloat16),
            pltpu.SMEM((NTV * NTV,), jnp.int32),
        ],
        compiler_params=pltpu.CompilerParams(vmem_limit_bytes=24 * 1024 * 1024),
        name="virt_partial",
    )(tile_list, place, packed)


def shards(amplitudes, pair_list, tile_list):
    _, slot_dev, row_dev, width = amplitudes.shape
    far = lax.axis_size("far")
    near = lax.axis_size("near")
    pair_count = far * near
    vir_at = lax.axis_index("vir")
    sub_at = lax.axis_index("sub")
    in_tile = jnp.arange(width, dtype=jnp.int32)
    own_list = lax.dynamic_slice_in_dim(tile_list, vir_at * slot_dev, slot_dev, 0)
    own_rows = sub_at * row_dev + jnp.arange(row_dev, dtype=jnp.int32)
    own_lower = in_tile[None, :] <= own_rows[:, None]
    own_diagonal = own_list[:, 0] == own_list[:, 1]
    keep = jnp.logical_not(own_diagonal[:, None, None] & own_lower[None])
    masked = jnp.where(keep, amplitudes[0], jnp.zeros((), jnp.bfloat16))

    other = lax.ppermute(masked, "sub", [(0, 1), (1, 0)])
    is_first = sub_at == 0
    tiles = jnp.concatenate(
        [jnp.where(is_first, masked, other), jnp.where(is_first, other, masked)], axis=1
    )
    packed = sent_to_all(tiles, "vir").reshape(-1, width, width)

    chunk = slot_dev * row_dev * width // pair_count
    share = masked.reshape(pair_count, chunk // width, width)
    ids = jnp.pad(pair_list.astype(jnp.bfloat16), ((0, 0), (0, width - 2)))
    ids = jnp.broadcast_to(ids[None], (pair_count, 1, width))
    got = lax.all_to_all(
        jnp.concatenate([share, ids], axis=1), ("far", "near"), split_axis=0, concat_axis=0, tiled=True
    )
    pairs = got[:, -1, :2].astype(jnp.int32)
    rows = got[:, :-1].reshape(pair_count, chunk)
    local_gram = lax.dot_general(
        rows, rows, (((1,), (1,)), ((), ())), preferred_element_type=jnp.float32
    )
    gram_rows = local_gram.reshape(-1, width)

    place = jnp.stack([vir_at * slot_dev, sub_at]).astype(jnp.int32)
    part = virt_partial(tile_list, place, packed, slot_dev, row_dev)
    part = part.reshape(near, slot_dev * row_dev // near, width)
    gram_copies = jnp.broadcast_to(gram_rows, (near, *gram_rows.shape))
    near_parts = lax.all_to_all(
        jnp.concatenate([part, gram_copies], axis=1), "near", split_axis=0, concat_axis=0, tiled=True
    )
    near_sum = near_parts.sum(axis=0)
    total = sent_to_all(near_sum, "far").sum(axis=0)
    virt_rows = total[: -gram_rows.shape[0]]
    p_virt = sent_to_all(virt_rows, "near").reshape(slot_dev, row_dev, width)
    gram = lax.psum(total[-gram_rows.shape[0] :], ("vir", "sub")).reshape(pair_count, pair_count)
    return (p_virt, occ_density(gram, pairs))


def solution(mesh):
    groups, pair, vir, sub = (mesh.shape[name] for name in ("groups", "pair", "vir", "sub"))
    split = Mesh(
        mesh.devices.reshape(groups, pair // NEAR, NEAR, vir, sub),
        ("groups", "far", "near", "vir", "sub"),
    )
    in_specs = (
        P(("groups", "far", "near"), "vir", "sub", None),
        P(("groups", "far", "near"), None),
        P(),
    )
    out_specs = (P(("groups", "vir"), "sub", None), P("groups", None))
    return jax.shard_map(shards, mesh=split, in_specs=in_specs, out_specs=out_specs, check_vma=False)
```

```python
import jax
import jax.numpy as jnp
from jax import lax
from jax.experimental import pallas as pl
from jax.experimental.pallas import tpu as pltpu
from jax.sharding import Mesh
from jax.sharding import PartitionSpec as P


OCC = 256
NTV = 8
NEAR = 8


def sent_to_all(array, axis):
    copies = jnp.broadcast_to(array, (lax.axis_size(axis), *array.shape))
    return lax.all_to_all(copies, axis, split_axis=0, concat_axis=0, tiled=True)


def occurrences(pair_rows):
    orbital = jnp.concatenate([pair_rows[:, 0], pair_rows[:, 1]])
    partner = jnp.concatenate([pair_rows[:, 1], pair_rows[:, 0]])
    pair_count = pair_rows.shape[0]
    parity = jnp.concatenate(
        [jnp.ones((pair_count,), jnp.float32), -jnp.ones((pair_count,), jnp.float32)]
    )
    return (orbital, partner, parity)


def occ_density(pair_gram, pairs):
    orb, partner, sign = occurrences(pairs)
    doubled = jnp.tile(pair_gram, (2, 2))
    couple = jnp.where(
        partner[:, None] == partner[None, :], sign[:, None] * sign[None, :] * doubled, 0.0
    )
    orbitals = jnp.arange(OCC, dtype=jnp.int32)
    hot = (orb[:, None] == orbitals[None, :]).astype(jnp.float32)
    inner_sum = jnp.dot(couple, hot, precision=lax.Precision.HIGHEST)
    return -jnp.dot(hot.T, inner_sum, precision=lax.Precision.HIGHEST)


def virt_kernel(tiles_ref, place_ref, own_ref, other_ref, out_ref, whole_ref, slot_ref):
    slot_count, half_rows, width = own_ref.shape
    own_count = out_ref.shape[0]
    first = place_ref[0]
    half = place_ref[1]

    def note(s, carry):
        slot_ref[tiles_ref[s, 0] * NTV + tiles_ref[s, 1]] = s
        return carry

    lax.fori_loop(0, slot_count, note, 0)
    is_first = half == 0
    for r in range(NTV):
        for c in range(r, NTV):
            slot = slot_ref[r * NTV + c]
            mine = own_ref[slot]
            theirs = other_ref[slot]
            tile = jnp.concatenate(
                [jnp.where(is_first, mine, theirs), jnp.where(is_first, theirs, mine)], axis=0
            )
            turned = tile.T
            if r == c:
                whole_ref[r, :, c * width : (c + 1) * width] = tile - turned
            else:
                whole_ref[r, :, c * width : (c + 1) * width] = tile
                whole_ref[c, :, r * width : (r + 1) * width] = -turned
    for i in range(own_count):
        left = whole_ref[tiles_ref[first + i, 0], pl.ds(half * half_rows, half_rows), :]
        right = whole_ref[tiles_ref[first + i, 1]]
        out_ref[i] = lax.dot_general(
            left, right, (((1,), (1,)), ((), ())), preferred_element_type=jnp.float32
        )


def virt_partial(tile_list, place, own, other, own_count):
    _, half_rows, width = own.shape
    smem = pl.BlockSpec(memory_space=pltpu.SMEM)
    vmem = pl.BlockSpec(memory_space=pltpu.VMEM)
    return pl.pallas_call(
        virt_kernel,
        out_shape=jax.ShapeDtypeStruct((own_count, half_rows, width), jnp.float32),
        in_specs=[smem, smem, vmem, vmem],
        out_specs=vmem,
        scratch_shapes=[
            pltpu.VMEM((NTV, width, NTV * width), jnp.bfloat16),
            pltpu.SMEM((NTV * NTV,), jnp.int32),
        ],
        compiler_params=pltpu.CompilerParams(vmem_limit_bytes=24 * 1024 * 1024),
        name="virt_partial",
    )(tile_list, place, own, other)


def shards(amplitudes, pair_list, tile_list):
    _, slot_dev, row_dev, width = amplitudes.shape
    far = lax.axis_size("far")
    near = lax.axis_size("near")
    pair_count = far * near
    vir_at = lax.axis_index("vir")
    sub_at = lax.axis_index("sub")
    in_tile = jnp.arange(width, dtype=jnp.int32)
    own_list = lax.dynamic_slice_in_dim(tile_list, vir_at * slot_dev, slot_dev, 0)
    own_rows = sub_at * row_dev + jnp.arange(row_dev, dtype=jnp.int32)
    own_lower = in_tile[None, :] <= own_rows[:, None]
    own_diagonal = own_list[:, 0] == own_list[:, 1]
    keep = jnp.logical_not(own_diagonal[:, None, None] & own_lower[None])
    masked = jnp.where(keep, amplitudes[0], jnp.zeros((), jnp.bfloat16))

    share_rows = row_dev // pair_count
    share = masked.reshape(slot_dev, pair_count, share_rows, width)
    share = jnp.transpose(share, (1, 2, 0, 3)).reshape(pair_count, share_rows, slot_dev * width)
    ids = jnp.pad(pair_list.astype(jnp.bfloat16), ((0, share_rows - 1), (0, width - 2)))
    ids = jnp.broadcast_to(ids[None], (pair_count, share_rows, width))
    got = lax.all_to_all(
        jnp.concatenate([share, ids], axis=2),
        ("far", "near"),
        split_axis=0,
        concat_axis=0,
        tiled=True,
    )
    own = lax.all_gather(masked, "vir", axis=0, tiled=True)
    other = lax.ppermute(own, "sub", [(0, 1), (1, 0)])
    place = jnp.stack([vir_at * slot_dev, sub_at]).astype(jnp.int32)
    part = virt_partial(tile_list, place, own, other, slot_dev)
    chunk = slot_dev * row_dev // near
    near_parts = lax.all_to_all(
        part.reshape(near, chunk, width), "near", split_axis=0, concat_axis=0, tiled=True
    )
    near_sum = near_parts.sum(axis=0)

    pairs = got[:, 0, slot_dev * width : slot_dev * width + 2].astype(jnp.int32)
    rows = got[:, :, : slot_dev * width].reshape(pair_count, share_rows * slot_dev * width)
    local_gram = lax.dot_general(
        rows, rows, (((1,), (1,)), ((), ())), preferred_element_type=jnp.float32
    )
    gram_rows = lax.psum(local_gram.reshape(-1, width), ("vir", "sub"))

    total = sent_to_all(jnp.concatenate([near_sum, gram_rows], axis=0), "far").sum(axis=0)
    spread = sent_to_all(total, "near")
    p_virt = spread[:, :chunk].reshape(slot_dev, row_dev, width)
    gram = spread[:, chunk:].sum(axis=0).reshape(pair_count, pair_count)
    return (p_virt, occ_density(gram, pairs))


def solution(mesh):
    groups, pair, vir, sub = (mesh.shape[name] for name in ("groups", "pair", "vir", "sub"))
    split = Mesh(
        mesh.devices.reshape(groups, pair // NEAR, NEAR, vir, sub),
        ("groups", "far", "near", "vir", "sub"),
    )
    in_specs = (
        P(("groups", "far", "near"), "vir", "sub", None),
        P(("groups", "far", "near"), None),
        P(),
    )
    out_specs = (P(("groups", "vir"), "sub", None), P("groups", None))
    return jax.shard_map(shards, mesh=split, in_specs=in_specs, out_specs=out_specs, check_vma=False)
```

```python
import jax
import jax.numpy as jnp
from jax import lax
from jax.experimental import pallas as pl
from jax.experimental.pallas import tpu as pltpu
from jax.sharding import Mesh
from jax.sharding import PartitionSpec as P


OCC = 256
NTV = 8
NEAR = 8


def sent_to_all(array, axis):
    copies = jnp.broadcast_to(array, (lax.axis_size(axis), *array.shape))
    return lax.all_to_all(copies, axis, split_axis=0, concat_axis=0, tiled=True)


def finish_kernel(spread_ref, columns_ref, rows_ref, virt_ref, occ_ref):
    near, _, width = spread_ref.shape
    chunk = virt_ref.shape[0] // near
    pair_count = columns_ref.shape[0]
    packed = spread_ref[0, chunk:, :]
    for k in range(1, near):
        packed = packed + spread_ref[k, chunk:, :]
    gram = jnp.concatenate(
        [packed[:, k : k + pair_count] for k in range(0, width, pair_count)], axis=0
    )
    signed = jnp.concatenate(
        [jnp.concatenate([gram, -gram], axis=1), jnp.concatenate([-gram, gram], axis=1)], axis=0
    )
    columns = columns_ref[...]
    rows = rows_ref[...]
    orb_column = jnp.concatenate([columns[:, 0:1], columns[:, 1:2]], axis=0)
    partner_column = jnp.concatenate([columns[:, 1:2], columns[:, 0:1]], axis=0)
    orb_row = jnp.concatenate([rows[0:1], rows[1:2]], axis=1)
    partner_row = jnp.concatenate([rows[1:2], rows[0:1]], axis=1)
    couple = jnp.where(partner_column == partner_row, signed, 0.0)
    hot_shape = (2 * pair_count, OCC)
    hot = (orb_column == lax.broadcasted_iota(jnp.int32, hot_shape, 1)).astype(jnp.float32)
    turned = (orb_row == lax.broadcasted_iota(jnp.int32, hot_shape[::-1], 0)).astype(jnp.float32)
    inner = jnp.dot(couple, hot, precision=lax.Precision.HIGHEST)
    occ_ref[...] = -jnp.dot(turned, inner, precision=lax.Precision.HIGHEST)
    for k in range(near):
        virt_ref[k * chunk : (k + 1) * chunk] = spread_ref[k, :chunk, :]


def finish(spread, pairs, chunk):
    near, _, width = spread.shape
    vmem = pl.BlockSpec(memory_space=pltpu.VMEM)
    return pl.pallas_call(
        finish_kernel,
        out_shape=(
            jax.ShapeDtypeStruct((near * chunk, width), jnp.float32),
            jax.ShapeDtypeStruct((OCC, OCC), jnp.float32),
        ),
        in_specs=[vmem, vmem, vmem],
        out_specs=(vmem, vmem),
        compiler_params=pltpu.CompilerParams(vmem_limit_bytes=8 * 1024 * 1024),
        name="finish",
    )(spread, *pairs)


def virt_kernel(tiles_ref, place_ref, own_ref, other_ref, out_ref, whole_ref, slot_ref):
    slot_count, half_rows, width = own_ref.shape
    own_count = out_ref.shape[0]
    first = place_ref[0]
    half = place_ref[1]

    def note(s, carry):
        slot_ref[tiles_ref[s, 0] * NTV + tiles_ref[s, 1]] = s
        return carry

    lax.fori_loop(0, slot_count, note, 0)
    is_first = half == 0
    for r in range(NTV):
        for c in range(r, NTV):
            slot = slot_ref[r * NTV + c]
            mine = own_ref[slot]
            theirs = other_ref[slot]
            tile = jnp.concatenate(
                [jnp.where(is_first, mine, theirs), jnp.where(is_first, theirs, mine)], axis=0
            )
            turned = tile.T
            if r == c:
                whole_ref[r, :, c * width : (c + 1) * width] = tile - turned
            else:
                whole_ref[r, :, c * width : (c + 1) * width] = tile
                whole_ref[c, :, r * width : (r + 1) * width] = -turned
    for i in range(own_count):
        left = whole_ref[tiles_ref[first + i, 0], pl.ds(half * half_rows, half_rows), :]
        right = whole_ref[tiles_ref[first + i, 1]]
        out_ref[i] = lax.dot_general(
            left, right, (((1,), (1,)), ((), ())), preferred_element_type=jnp.float32
        )


def virt_partial(tile_list, place, own, other, own_count):
    _, half_rows, width = own.shape
    smem = pl.BlockSpec(memory_space=pltpu.SMEM)
    vmem = pl.BlockSpec(memory_space=pltpu.VMEM)
    return pl.pallas_call(
        virt_kernel,
        out_shape=jax.ShapeDtypeStruct((own_count, half_rows, width), jnp.float32),
        in_specs=[smem, smem, vmem, vmem],
        out_specs=vmem,
        scratch_shapes=[
            pltpu.VMEM((NTV, width, NTV * width), jnp.bfloat16),
            pltpu.SMEM((NTV * NTV,), jnp.int32),
        ],
        compiler_params=pltpu.CompilerParams(vmem_limit_bytes=24 * 1024 * 1024),
        name="virt_partial",
    )(tile_list, place, own, other)


def shards(amplitudes, pair_list, tile_list):
    _, slot_dev, row_dev, width = amplitudes.shape
    far = lax.axis_size("far")
    near = lax.axis_size("near")
    pair_count = far * near
    vir_at = lax.axis_index("vir")
    sub_at = lax.axis_index("sub")
    in_tile = jnp.arange(width, dtype=jnp.int32)
    own_list = lax.dynamic_slice_in_dim(tile_list, vir_at * slot_dev, slot_dev, 0)
    own_rows = sub_at * row_dev + jnp.arange(row_dev, dtype=jnp.int32)
    own_lower = in_tile[None, :] <= own_rows[:, None]
    own_diagonal = own_list[:, 0] == own_list[:, 1]
    keep = jnp.logical_not(own_diagonal[:, None, None] & own_lower[None])
    masked = jnp.where(keep, amplitudes[0], jnp.zeros((), jnp.bfloat16))

    share_rows = row_dev // pair_count
    share = masked.reshape(slot_dev, pair_count, share_rows, width)
    share = jnp.transpose(share, (1, 2, 0, 3)).reshape(pair_count, share_rows, slot_dev * width)
    ids = jnp.pad(pair_list.astype(jnp.bfloat16), ((0, share_rows - 1), (0, width - 2)))
    ids = jnp.broadcast_to(ids[None], (pair_count, share_rows, width))
    got = lax.all_to_all(
        jnp.concatenate([share, ids], axis=2),
        ("far", "near"),
        split_axis=0,
        concat_axis=0,
        tiled=True,
    )
    own = lax.all_gather(masked, "vir", axis=0, tiled=True)
    other = lax.ppermute(own, "sub", [(0, 1), (1, 0)])
    place = jnp.stack([vir_at * slot_dev, sub_at]).astype(jnp.int32)
    part = virt_partial(tile_list, place, own, other, slot_dev)
    pairs = got[:, 0, slot_dev * width : slot_dev * width + 2].astype(jnp.int32)
    rows = got[:, :, : slot_dev * width].reshape(pair_count, share_rows * slot_dev * width)
    local_gram = lax.dot_general(
        rows, rows, (((1,), (1,)), ((), ())), preferred_element_type=jnp.float32
    )
    blocks = width // pair_count
    packed_gram = local_gram.reshape(blocks, pair_count // blocks, pair_count)
    packed_gram = jnp.transpose(packed_gram, (1, 0, 2)).reshape(-1, width)
    packed_gram, *pairs = lax.optimization_barrier((packed_gram, pairs, pairs.T))
    gram_rows = sent_to_all(packed_gram, ("vir", "sub")).sum(axis=0)

    part, gram_rows = lax.optimization_barrier((part, gram_rows))
    chunk = slot_dev * row_dev // near
    near_parts = lax.all_to_all(
        part.reshape(near, chunk, width), "near", split_axis=0, concat_axis=0, tiled=True
    )
    near_sum = near_parts.sum(axis=0)
    total = sent_to_all(jnp.concatenate([near_sum, gram_rows], axis=0), "far").sum(axis=0)
    spread = sent_to_all(total, "near")
    virt_rows, p_occ = finish(spread, pairs, chunk)
    return (virt_rows.reshape(slot_dev, row_dev, width), p_occ)


def solution(mesh):
    groups, pair, vir, sub = (mesh.shape[name] for name in ("groups", "pair", "vir", "sub"))
    split = Mesh(
        mesh.devices.reshape(groups, pair // NEAR, NEAR, vir, sub),
        ("groups", "far", "near", "vir", "sub"),
    )
    in_specs = (
        P(("groups", "far", "near"), "vir", "sub", None),
        P(("groups", "far", "near"), None),
        P(),
    )
    out_specs = (P(("groups", "vir"), "sub", None), P("groups", None))
    return jax.shard_map(shards, mesh=split, in_specs=in_specs, out_specs=out_specs, check_vma=False)
```

```python
import jax
import jax.numpy as jnp
from jax import lax
from jax.experimental import pallas as pl
from jax.experimental.pallas import tpu as pltpu
from jax.sharding import Mesh
from jax.sharding import PartitionSpec as P


OCC = 256
NTV = 8
NEAR = 8
GRAIN = 8
STEPS = 256.0
TOP = 32767.0
FLOOR = 2.0**-120


def coded(values):
    largest = jnp.max(jnp.abs(values), axis=1, keepdims=True)
    k = jnp.floor(jnp.log2(jnp.maximum(largest, FLOOR)) * STEPS) + 2.0
    return (values * (jnp.exp2(k * (-1.0 / STEPS)) * TOP), k)


def rounded(values):
    return jnp.clip(jnp.floor(values + 0.5), -TOP, TOP)


def as_row(column, width):
    shape = (column.shape[0], width)
    here = lax.broadcasted_iota(jnp.int32, shape, 0) == lax.broadcasted_iota(jnp.int32, shape, 1)
    return jnp.sum(jnp.where(here, column, 0.0), axis=0, keepdims=True)


def as_column(row, count):
    shape = (count, row.shape[1])
    here = lax.broadcasted_iota(jnp.int32, shape, 0) == lax.broadcasted_iota(jnp.int32, shape, 1)
    return jnp.sum(jnp.where(here, row, 0.0), axis=1, keepdims=True)


def scale_of(row, count):
    return jnp.exp2(as_column(row, count) * (1.0 / STEPS)) * (1.0 / TOP)


def message(values, gram=None):
    _, width = values.shape
    codes, k = coded(values)
    parts = [rounded(codes)]
    scales = [as_row(k, width)]
    if gram is not None:
        gram_codes, gram_k = coded(gram)
        high = rounded(gram_codes)
        parts += [high, rounded((gram_codes - high) * TOP)]
        scales.append(as_row(gram_k, width))
    spare = jnp.zeros((GRAIN - len(scales), width), jnp.float32)
    whole = jnp.concatenate([parts[0], jnp.concatenate([*scales, spare], axis=0), *parts[1:]], axis=0)
    return whole.astype(jnp.int32).astype(jnp.int16)


def opened(block, count, with_gram):
    words = block.astype(jnp.int32).astype(jnp.float32)
    values = words[:count] * scale_of(words[count : count + 1], count)
    if not with_gram:
        return (values, None)
    high = words[count + GRAIN : count + 2 * GRAIN]
    low = words[count + 2 * GRAIN : count + 3 * GRAIN]
    gram = (high + low * (1.0 / TOP)) * scale_of(words[count + 1 : count + 2], GRAIN)
    return (values, gram)


def near_kernel(parts_ref, gram_ref, out_ref):
    count = parts_ref.shape[1] - GRAIN
    total, _ = opened(parts_ref[0], count, False)
    for k in range(1, parts_ref.shape[0]):
        total = total + opened(parts_ref[k], count, False)[0]
    block = message(total, gram_ref[...])
    for k in range(out_ref.shape[0]):
        out_ref[k] = block


def far_kernel(parts_ref, out_ref):
    count = parts_ref.shape[1] - 3 * GRAIN
    total, gram = opened(parts_ref[0], count, True)
    for k in range(1, parts_ref.shape[0]):
        more, more_gram = opened(parts_ref[k], count, True)
        total = total + more
        gram = gram + more_gram
    block = message(total, gram)
    for k in range(out_ref.shape[0]):
        out_ref[k] = block


def finish_kernel(spread_ref, columns_ref, rows_ref, virt_ref, occ_ref):
    near, _, width = spread_ref.shape
    chunk = virt_ref.shape[0] // near
    pair_count = columns_ref.shape[0]
    packed = None
    for k in range(near):
        values, gram = opened(spread_ref[k], chunk, True)
        virt_ref[k * chunk : (k + 1) * chunk] = values
        packed = gram if packed is None else packed + gram
    gram = jnp.concatenate(
        [packed[:, k : k + pair_count] for k in range(0, width, pair_count)], axis=0
    )
    signed = jnp.concatenate(
        [jnp.concatenate([gram, -gram], axis=1), jnp.concatenate([-gram, gram], axis=1)], axis=0
    )
    columns = columns_ref[...]
    rows = rows_ref[...]
    orb_column = jnp.concatenate([columns[:, 0:1], columns[:, 1:2]], axis=0)
    partner_column = jnp.concatenate([columns[:, 1:2], columns[:, 0:1]], axis=0)
    orb_row = jnp.concatenate([rows[0:1], rows[1:2]], axis=1)
    partner_row = jnp.concatenate([rows[1:2], rows[0:1]], axis=1)
    couple = jnp.where(partner_column == partner_row, signed, 0.0)
    hot_shape = (2 * pair_count, OCC)
    hot = (orb_column == lax.broadcasted_iota(jnp.int32, hot_shape, 1)).astype(jnp.float32)
    turned = (orb_row == lax.broadcasted_iota(jnp.int32, hot_shape[::-1], 0)).astype(jnp.float32)
    inner = jnp.dot(couple, hot, precision=lax.Precision.HIGHEST)
    occ_ref[...] = -jnp.dot(turned, inner, precision=lax.Precision.HIGHEST)


def in_vmem(kernel, out_shape, *operands):
    vmem = pl.BlockSpec(memory_space=pltpu.VMEM)
    return pl.pallas_call(
        kernel,
        out_shape=out_shape,
        in_specs=[vmem] * len(operands),
        out_specs=jax.tree.map(lambda _: vmem, out_shape),
        compiler_params=pltpu.CompilerParams(vmem_limit_bytes=8 * 1024 * 1024),
    )(*operands)


def virt_kernel(tiles_ref, place_ref, own_ref, other_ref, out_ref, whole_ref, part_ref, slot_ref):
    slot_count, half_rows, width = own_ref.shape
    own_count = part_ref.shape[0] // half_rows
    first = place_ref[0]
    half = place_ref[1]

    def note(s, carry):
        slot_ref[tiles_ref[s, 0] * NTV + tiles_ref[s, 1]] = s
        return carry

    lax.fori_loop(0, slot_count, note, 0)
    is_first = half == 0
    for r in range(NTV):
        for c in range(r, NTV):
            slot = slot_ref[r * NTV + c]
            mine = own_ref[slot]
            theirs = other_ref[slot]
            tile = jnp.concatenate(
                [jnp.where(is_first, mine, theirs), jnp.where(is_first, theirs, mine)], axis=0
            )
            turned = tile.T
            if r == c:
                whole_ref[r, :, c * width : (c + 1) * width] = tile - turned
            else:
                whole_ref[r, :, c * width : (c + 1) * width] = tile
                whole_ref[c, :, r * width : (r + 1) * width] = -turned
    for i in range(own_count):
        left = whole_ref[tiles_ref[first + i, 0], pl.ds(half * half_rows, half_rows), :]
        right = whole_ref[tiles_ref[first + i, 1]]
        part_ref[i * half_rows : (i + 1) * half_rows] = lax.dot_general(
            left, right, (((1,), (1,)), ((), ())), preferred_element_type=jnp.float32
        )
    chunk = part_ref.shape[0] // out_ref.shape[0]
    for k in range(out_ref.shape[0]):
        out_ref[k] = message(part_ref[k * chunk : (k + 1) * chunk])


def virt_partial(tile_list, place, own, other, own_count, near):
    _, half_rows, width = own.shape
    rows = own_count * half_rows
    smem = pl.BlockSpec(memory_space=pltpu.SMEM)
    vmem = pl.BlockSpec(memory_space=pltpu.VMEM)
    return pl.pallas_call(
        virt_kernel,
        out_shape=jax.ShapeDtypeStruct((near, rows // near + GRAIN, width), jnp.int16),
        in_specs=[smem, smem, vmem, vmem],
        out_specs=vmem,
        scratch_shapes=[
            pltpu.VMEM((NTV, width, NTV * width), jnp.bfloat16),
            pltpu.VMEM((rows, width), jnp.float32),
            pltpu.SMEM((NTV * NTV,), jnp.int32),
        ],
        compiler_params=pltpu.CompilerParams(vmem_limit_bytes=24 * 1024 * 1024),
        name="virt_partial",
    )(tile_list, place, own, other)


def shards(amplitudes, pair_list, tile_list):
    _, slot_dev, row_dev, width = amplitudes.shape
    far = lax.axis_size("far")
    near = lax.axis_size("near")
    pair_count = far * near
    vir_at = lax.axis_index("vir")
    sub_at = lax.axis_index("sub")
    in_tile = jnp.arange(width, dtype=jnp.int32)
    own_list = lax.dynamic_slice_in_dim(tile_list, vir_at * slot_dev, slot_dev, 0)
    own_rows = sub_at * row_dev + jnp.arange(row_dev, dtype=jnp.int32)
    own_lower = in_tile[None, :] <= own_rows[:, None]
    own_diagonal = own_list[:, 0] == own_list[:, 1]
    keep = jnp.logical_not(own_diagonal[:, None, None] & own_lower[None])
    masked = jnp.where(keep, amplitudes[0], jnp.zeros((), jnp.bfloat16))

    share_rows = row_dev // pair_count
    share = masked.reshape(slot_dev, pair_count, share_rows, width)
    share = jnp.transpose(share, (1, 2, 0, 3)).reshape(pair_count, share_rows, slot_dev * width)
    ids = jnp.pad(pair_list.astype(jnp.bfloat16), ((0, share_rows - 1), (0, width - 2)))
    ids = jnp.broadcast_to(ids[None], (pair_count, share_rows, width))
    got = lax.all_to_all(
        jnp.concatenate([share, ids], axis=2),
        ("far", "near"),
        split_axis=0,
        concat_axis=0,
        tiled=True,
    )
    own = lax.all_gather(masked, "vir", axis=0, tiled=True)
    other = lax.ppermute(own, "sub", [(0, 1), (1, 0)])
    place = jnp.stack([vir_at * slot_dev, sub_at]).astype(jnp.int32)
    part = virt_partial(tile_list, place, own, other, slot_dev, near)
    pairs = got[:, 0, slot_dev * width : slot_dev * width + 2].astype(jnp.int32)
    rows = got[:, :, : slot_dev * width].reshape(pair_count, share_rows * slot_dev * width)
    local_gram = lax.dot_general(
        rows, rows, (((1,), (1,)), ((), ())), preferred_element_type=jnp.float32
    )
    blocks = width // pair_count
    packed_gram = local_gram.reshape(blocks, pair_count // blocks, pair_count)
    packed_gram = jnp.transpose(packed_gram, (1, 0, 2)).reshape(-1, width)
    columns, rows = pairs, pairs.T
    chunk = slot_dev * row_dev // near
    near_parts = lax.all_to_all(part, "near", split_axis=0, concat_axis=0, tiled=True)
    gram_rows = lax.psum(packed_gram, ("vir", "sub"))
    long_rows = chunk + 3 * GRAIN
    far_block = in_vmem(
        near_kernel, jax.ShapeDtypeStruct((far, long_rows, width), jnp.int16), near_parts, gram_rows
    )
    far_block, columns, rows = lax.optimization_barrier((far_block, columns, rows))
    far_parts = lax.all_to_all(far_block, "far", split_axis=0, concat_axis=0, tiled=True)
    last_block = in_vmem(
        far_kernel, jax.ShapeDtypeStruct((near, long_rows, width), jnp.int16), far_parts
    )
    spread = lax.all_to_all(last_block, "near", split_axis=0, concat_axis=0, tiled=True)
    virt_rows, p_occ = in_vmem(
        finish_kernel,
        (
            jax.ShapeDtypeStruct((near * chunk, width), jnp.float32),
            jax.ShapeDtypeStruct((OCC, OCC), jnp.float32),
        ),
        spread,
        columns,
        rows,
    )
    return (virt_rows.reshape(slot_dev, row_dev, width), p_occ)


def solution(mesh):
    groups, pair, vir, sub = (mesh.shape[name] for name in ("groups", "pair", "vir", "sub"))
    split = Mesh(
        mesh.devices.reshape(groups, pair // NEAR, NEAR, vir, sub),
        ("groups", "far", "near", "vir", "sub"),
    )
    in_specs = (
        P(("groups", "far", "near"), "vir", "sub", None),
        P(("groups", "far", "near"), None),
        P(),
    )
    out_specs = (P(("groups", "vir"), "sub", None), P("groups", None))
    return jax.shard_map(shards, mesh=split, in_specs=in_specs, out_specs=out_specs, check_vma=False)
```

```python
import jax
import jax.numpy as jnp
from jax import lax
from jax.experimental import pallas as pl
from jax.experimental.pallas import tpu as pltpu
from jax.sharding import Mesh
from jax.sharding import PartitionSpec as P


OCC = 256
NTV = 8
NEAR = 8
GRAIN = 8
STEPS = 256.0
TOP = 32767.0
FLOOR = 2.0**-120


def coded(values):
    largest = jnp.max(jnp.abs(values), axis=1, keepdims=True)
    k = jnp.floor(jnp.log2(jnp.maximum(largest, FLOOR)) * STEPS) + 2.0
    return (values * (jnp.exp2(k * (-1.0 / STEPS)) * TOP), k)


def rounded(values):
    return jnp.clip(jnp.floor(values + 0.5), -TOP, TOP)


def as_row(column, width):
    shape = (column.shape[0], width)
    here = lax.broadcasted_iota(jnp.int32, shape, 0) == lax.broadcasted_iota(jnp.int32, shape, 1)
    return jnp.sum(jnp.where(here, column, 0.0), axis=0, keepdims=True)


def as_column(row, count):
    shape = (count, row.shape[1])
    here = lax.broadcasted_iota(jnp.int32, shape, 0) == lax.broadcasted_iota(jnp.int32, shape, 1)
    return jnp.sum(jnp.where(here, row, 0.0), axis=1, keepdims=True)


def scale_of(row, count):
    return jnp.exp2(as_column(row, count) * (1.0 / STEPS)) * (1.0 / TOP)


def message(values, gram=None, ids=None):
    _, width = values.shape
    codes, k = coded(values)
    parts = [rounded(codes)]
    scales = [as_row(k, width)]
    if gram is not None:
        gram_codes, gram_k = coded(gram)
        high = rounded(gram_codes)
        parts += [high, rounded((gram_codes - high) * TOP)]
        scales += [as_row(gram_k, width), ids]
    spare = jnp.zeros((GRAIN - len(scales), width), jnp.float32)
    whole = jnp.concatenate([parts[0], jnp.concatenate([*scales, spare], axis=0), *parts[1:]], axis=0)
    return whole.astype(jnp.int32).astype(jnp.int16)


def opened(block, count, with_gram):
    words = block.astype(jnp.int32).astype(jnp.float32)
    values = words[:count] * scale_of(words[count : count + 1], count)
    if not with_gram:
        return (values, None, None)
    high = words[count + GRAIN : count + 2 * GRAIN]
    low = words[count + 2 * GRAIN : count + 3 * GRAIN]
    gram = (high + low * (1.0 / TOP)) * scale_of(words[count + 1 : count + 2], GRAIN)
    return (values, gram, words[count + 2 : count + 3])


def near_kernel(parts_ref, gram_ref, ids_ref, out_ref):
    count = parts_ref.shape[1] - GRAIN
    total, _, _ = opened(parts_ref[0], count, False)
    for k in range(1, parts_ref.shape[0]):
        total = total + opened(parts_ref[k], count, False)[0]
    block = message(total, gram_ref[...], ids_ref[...])
    for k in range(out_ref.shape[0]):
        out_ref[k] = block


def far_kernel(parts_ref, out_ref):
    count = parts_ref.shape[1] - 3 * GRAIN
    total, gram, ids = opened(parts_ref[0], count, True)
    for k in range(1, parts_ref.shape[0]):
        more, more_gram, more_ids = opened(parts_ref[k], count, True)
        total = total + more
        gram = gram + more_gram
        ids = ids + more_ids
    block = message(total, gram, ids)
    for k in range(out_ref.shape[0]):
        out_ref[k] = block


def finish_kernel(spread_ref, virt_ref, occ_ref):
    near, _, width = spread_ref.shape
    chunk = virt_ref.shape[0] // near
    pair_count = width // 4
    packed, ids = 0.0, 0.0
    for k in range(near):
        values, gram, some_ids = opened(spread_ref[k], chunk, True)
        virt_ref[k * chunk : (k + 1) * chunk] = values
        packed = packed + gram
        ids = ids + some_ids
    gram = jnp.concatenate(
        [packed[:, k : k + pair_count] for k in range(0, width, pair_count)], axis=0
    )
    signed = jnp.concatenate(
        [jnp.concatenate([gram, -gram], axis=1), jnp.concatenate([-gram, gram], axis=1)], axis=0
    )
    orb_row = ids[:, : 2 * pair_count]
    partner_row = ids[:, 2 * pair_count :]
    orb_column = as_column(orb_row, 2 * pair_count)
    partner_column = as_column(partner_row, 2 * pair_count)
    couple = jnp.where(partner_column == partner_row, signed, 0.0)
    hot_shape = (2 * pair_count, OCC)
    across = lax.broadcasted_iota(jnp.int32, hot_shape, 1).astype(jnp.float32)
    down = lax.broadcasted_iota(jnp.int32, hot_shape[::-1], 0).astype(jnp.float32)
    hot = (orb_column == across).astype(jnp.float32)
    turned = (orb_row == down).astype(jnp.float32)
    inner = jnp.dot(couple, hot, precision=lax.Precision.HIGHEST)
    occ_ref[...] = -jnp.dot(turned, inner, precision=lax.Precision.HIGHEST)


def in_vmem(kernel, out_shape, *operands):
    vmem = pl.BlockSpec(memory_space=pltpu.VMEM)
    return pl.pallas_call(
        kernel,
        out_shape=out_shape,
        in_specs=[vmem] * len(operands),
        out_specs=jax.tree.map(lambda _: vmem, out_shape),
        compiler_params=pltpu.CompilerParams(vmem_limit_bytes=8 * 1024 * 1024),
    )(*operands)


def virt_kernel(tiles_ref, place_ref, own_ref, other_ref, out_ref, whole_ref, part_ref, slot_ref):
    slot_count, half_rows, width = own_ref.shape
    own_count = part_ref.shape[0] // half_rows
    vir_at = place_ref[0]
    half = place_ref[1]
    own_tiles = own_count
    holders = slot_count // own_tiles
    first = vir_at * own_tiles

    def note(s, carry):
        steps = lax.rem(vir_at + holders - s // own_tiles, holders)
        where = steps * own_tiles + lax.rem(s, own_tiles)
        slot_ref[tiles_ref[s, 0] * NTV + tiles_ref[s, 1]] = where
        return carry

    lax.fori_loop(0, slot_count, note, 0)
    is_first = half == 0
    shape = (width, width)
    upper = lax.broadcasted_iota(jnp.int32, shape, 0) < lax.broadcasted_iota(jnp.int32, shape, 1)
    for r in range(NTV):
        for c in range(r, NTV):
            slot = slot_ref[r * NTV + c]
            mine = own_ref[slot]
            theirs = other_ref[slot]
            tile = jnp.concatenate(
                [jnp.where(is_first, mine, theirs), jnp.where(is_first, theirs, mine)], axis=0
            )
            if r == c:
                tile = jnp.where(upper, tile, jnp.zeros_like(tile))
            turned = tile.T
            if r == c:
                whole_ref[r, :, c * width : (c + 1) * width] = tile - turned
            else:
                whole_ref[r, :, c * width : (c + 1) * width] = tile
                whole_ref[c, :, r * width : (r + 1) * width] = -turned
    for i in range(own_count):
        left = whole_ref[tiles_ref[first + i, 0], pl.ds(half * half_rows, half_rows), :]
        right = whole_ref[tiles_ref[first + i, 1]]
        part_ref[i * half_rows : (i + 1) * half_rows] = lax.dot_general(
            left, right, (((1,), (1,)), ((), ())), preferred_element_type=jnp.float32
        )
    chunk = part_ref.shape[0] // out_ref.shape[0]
    for k in range(out_ref.shape[0]):
        out_ref[k] = message(part_ref[k * chunk : (k + 1) * chunk])


def virt_partial(tile_list, place, own, other, own_count, near):
    _, half_rows, width = own.shape
    rows = own_count * half_rows
    smem = pl.BlockSpec(memory_space=pltpu.SMEM)
    vmem = pl.BlockSpec(memory_space=pltpu.VMEM)
    return pl.pallas_call(
        virt_kernel,
        out_shape=jax.ShapeDtypeStruct((near, rows // near + GRAIN, width), jnp.int16),
        in_specs=[smem, smem, vmem, vmem],
        out_specs=vmem,
        scratch_shapes=[
            pltpu.VMEM((NTV, width, NTV * width), jnp.bfloat16),
            pltpu.VMEM((rows, width), jnp.float32),
            pltpu.SMEM((NTV * NTV,), jnp.int32),
        ],
        compiler_params=pltpu.CompilerParams(vmem_limit_bytes=24 * 1024 * 1024),
        name="virt_partial",
    )(tile_list, place, own, other)


def shards(amplitudes, pair_list, tile_list):
    _, slot_dev, row_dev, width = amplitudes.shape
    far = lax.axis_size("far")
    near = lax.axis_size("near")
    pair_count = far * near
    vir_at = lax.axis_index("vir")
    sub_at = lax.axis_index("sub")
    pair_at = lax.axis_index(("far", "near"))
    mine = amplitudes[0]
    holders = lax.axis_size("vir")

    pieces = [mine]
    for step in range(1, holders):
        hops = [(k, (k + step) % holders) for k in range(holders)]
        pieces.append(lax.ppermute(mine, "vir", hops))
    share_rows = row_dev // pair_count
    share = mine.reshape(slot_dev, pair_count, share_rows, width)
    share = jnp.transpose(share, (1, 2, 0, 3)).reshape(pair_count, share_rows, slot_dev * width)
    got = lax.all_to_all(share, ("far", "near"), split_axis=0, concat_axis=0, tiled=True)
    own = jnp.concatenate(pieces, axis=0)
    other = lax.ppermute(own, "sub", [(0, 1), (1, 0)])
    place = jnp.stack([vir_at, sub_at]).astype(jnp.int32)
    part = virt_partial(tile_list, place, own, other, slot_dev, near)
    own_list = lax.dynamic_slice_in_dim(tile_list, vir_at * slot_dev, slot_dev, 0)
    row = sub_at * row_dev + pair_at * share_rows + jnp.arange(share_rows, dtype=jnp.int32)
    column = jnp.arange(width, dtype=jnp.int32)
    lower = column[None, None, :] <= row[:, None, None]
    diagonal = (own_list[:, 0] == own_list[:, 1])[None, :, None]
    keep = jnp.logical_not(diagonal & lower).reshape(1, share_rows * slot_dev * width)
    rows = got.reshape(pair_count, share_rows * slot_dev * width)
    local_gram = lax.dot_general(
        jnp.where(keep, rows, jnp.zeros((), rows.dtype)),
        rows,
        (((1,), (1,)), ((), ())),
        preferred_element_type=jnp.float32,
    )
    lane = jnp.arange(width, dtype=jnp.int32)
    quarter = lane // pair_count
    swapped = (quarter == 1) | (quarter == 2)
    own_ids = jnp.where(swapped, pair_list[0, 1], pair_list[0, 0]).astype(jnp.float32)
    ids = jnp.where(lane % pair_count == pair_at, own_ids, 0.0)[None]
    blocks = width // pair_count
    packed_gram = local_gram.reshape(blocks, pair_count // blocks, pair_count)
    packed_gram = jnp.transpose(packed_gram, (1, 0, 2)).reshape(-1, width)
    chunk = slot_dev * row_dev // near
    near_parts = lax.all_to_all(part, "near", split_axis=0, concat_axis=0, tiled=True)
    gram_rows = lax.psum(packed_gram, ("vir", "sub"))
    long_rows = chunk + 3 * GRAIN
    far_block = in_vmem(
        near_kernel,
        jax.ShapeDtypeStruct((far, long_rows, width), jnp.int16),
        near_parts,
        gram_rows,
        ids,
    )
    far_parts = lax.all_to_all(far_block, "far", split_axis=0, concat_axis=0, tiled=True)
    last_block = in_vmem(
        far_kernel, jax.ShapeDtypeStruct((near, long_rows, width), jnp.int16), far_parts
    )
    spread = lax.all_to_all(last_block, "near", split_axis=0, concat_axis=0, tiled=True)
    virt_rows, p_occ = in_vmem(
        finish_kernel,
        (
            jax.ShapeDtypeStruct((near * chunk, width), jnp.float32),
            jax.ShapeDtypeStruct((OCC, OCC), jnp.float32),
        ),
        spread,
    )
    return (virt_rows.reshape(slot_dev, row_dev, width), p_occ)


def solution(mesh):
    groups, pair, vir, sub = (mesh.shape[name] for name in ("groups", "pair", "vir", "sub"))
    split = Mesh(
        mesh.devices.reshape(groups, pair // NEAR, NEAR, vir, sub),
        ("groups", "far", "near", "vir", "sub"),
    )
    in_specs = (
        P(("groups", "far", "near"), "vir", "sub", None),
        P(("groups", "far", "near"), None),
        P(),
    )
    out_specs = (P(("groups", "vir"), "sub", None), P("groups", None))
    return jax.shard_map(shards, mesh=split, in_specs=in_specs, out_specs=out_specs, check_vma=False)
```

```python
import jax
import jax.numpy as jnp
from jax import lax
from jax.experimental import pallas as pl
from jax.experimental.pallas import tpu as pltpu
from jax.sharding import Mesh
from jax.sharding import PartitionSpec as P


OCC = 256
NTV = 8
NEAR = 8
GRAIN = 8
STEPS = 256.0
TOP = 32767.0
FLOOR = 2.0**-120


def coded(values):
    largest = jnp.max(jnp.abs(values), axis=1, keepdims=True)
    k = jnp.floor(jnp.log2(jnp.maximum(largest, FLOOR)) * STEPS) + 2.0
    return (values * (jnp.exp2(k * (-1.0 / STEPS)) * TOP), k)


def rounded(values):
    return jnp.clip(jnp.floor(values + 0.5), -TOP, TOP)


def as_row(column, width):
    shape = (column.shape[0], width)
    here = lax.broadcasted_iota(jnp.int32, shape, 0) == lax.broadcasted_iota(jnp.int32, shape, 1)
    return jnp.sum(jnp.where(here, column, 0.0), axis=0, keepdims=True)


def as_column(row, count):
    shape = (count, row.shape[1])
    here = lax.broadcasted_iota(jnp.int32, shape, 0) == lax.broadcasted_iota(jnp.int32, shape, 1)
    return jnp.sum(jnp.where(here, row, 0.0), axis=1, keepdims=True)


def scale_of(row, count):
    return jnp.exp2(as_column(row, count) * (1.0 / STEPS)) * (1.0 / TOP)


def message(values, gram=None, ids=None):
    _, width = values.shape
    codes, k = coded(values)
    parts = [rounded(codes)]
    scales = [as_row(k, width)]
    if gram is not None:
        gram_codes, gram_k = coded(gram)
        high = rounded(gram_codes)
        parts += [high, rounded((gram_codes - high) * TOP)]
        scales += [as_row(gram_k, width), ids]
    spare = jnp.zeros((GRAIN - len(scales), width), jnp.float32)
    whole = jnp.concatenate([parts[0], jnp.concatenate([*scales, spare], axis=0), *parts[1:]], axis=0)
    return whole.astype(jnp.int32).astype(jnp.int16)


def opened(block, count, with_gram):
    words = block.astype(jnp.int32).astype(jnp.float32)
    values = words[:count] * scale_of(words[count : count + 1], count)
    if not with_gram:
        return (values, None, None)
    high = words[count + GRAIN : count + 2 * GRAIN]
    low = words[count + 2 * GRAIN : count + 3 * GRAIN]
    gram = (high + low * (1.0 / TOP)) * scale_of(words[count + 1 : count + 2], GRAIN)
    return (values, gram, words[count + 2 : count + 3])


def near_kernel(place_ref, pair_ref, parts_ref, gram_ref, out_ref):
    width = parts_ref.shape[2]
    pair_count = width // 4
    lane = lax.broadcasted_iota(jnp.int32, (1, width), 1)
    quarter = lane // pair_count
    swapped = (quarter == 1) | (quarter == 2)
    own_ids = jnp.where(swapped, pair_ref[:, 1:2], pair_ref[:, 0:1])
    ids = jnp.where(lane - quarter * pair_count == place_ref[2], own_ids, 0).astype(jnp.float32)
    count = parts_ref.shape[1] - GRAIN
    total, _, _ = opened(parts_ref[0], count, False)
    for k in range(1, parts_ref.shape[0]):
        total = total + opened(parts_ref[k], count, False)[0]
    block = message(total, gram_ref[...], ids)
    for k in range(out_ref.shape[0]):
        out_ref[k] = block


def far_kernel(parts_ref, out_ref):
    count = parts_ref.shape[1] - 3 * GRAIN
    total, gram, ids = opened(parts_ref[0], count, True)
    for k in range(1, parts_ref.shape[0]):
        more, more_gram, more_ids = opened(parts_ref[k], count, True)
        total = total + more
        gram = gram + more_gram
        ids = ids + more_ids
    block = message(total, gram, ids)
    for k in range(out_ref.shape[0]):
        out_ref[k] = block


def finish_kernel(spread_ref, virt_ref, occ_ref):
    near, _, width = spread_ref.shape
    chunk = virt_ref.shape[0] // near
    pair_count = width // 4
    packed, ids = 0.0, 0.0
    for k in range(near):
        values, gram, some_ids = opened(spread_ref[k], chunk, True)
        virt_ref[k * chunk : (k + 1) * chunk] = values
        packed = packed + gram
        ids = ids + some_ids
    gram = jnp.concatenate(
        [packed[:, k : k + pair_count] for k in range(0, width, pair_count)], axis=0
    )
    signed = jnp.concatenate(
        [jnp.concatenate([gram, -gram], axis=1), jnp.concatenate([-gram, gram], axis=1)], axis=0
    )
    orb_row = ids[:, : 2 * pair_count]
    partner_row = ids[:, 2 * pair_count :]
    orb_column = as_column(orb_row, 2 * pair_count)
    partner_column = as_column(partner_row, 2 * pair_count)
    couple = jnp.where(partner_column == partner_row, signed, 0.0)
    hot_shape = (2 * pair_count, OCC)
    across = lax.broadcasted_iota(jnp.int32, hot_shape, 1).astype(jnp.float32)
    down = lax.broadcasted_iota(jnp.int32, hot_shape[::-1], 0).astype(jnp.float32)
    hot = (orb_column == across).astype(jnp.float32)
    turned = (orb_row == down).astype(jnp.float32)
    inner = jnp.dot(couple, hot, precision=lax.Precision.HIGHEST)
    occ_ref[...] = -jnp.dot(turned, inner, precision=lax.Precision.HIGHEST)


def in_vmem(kernel, out_shape, *operands, place=None):
    vmem = pl.BlockSpec(memory_space=pltpu.VMEM)
    smem = pl.BlockSpec(memory_space=pltpu.SMEM)
    places = () if place is None else (place,)
    return pl.pallas_call(
        kernel,
        out_shape=out_shape,
        in_specs=[smem] * len(places) + [vmem] * len(operands),
        out_specs=jax.tree.map(lambda _: vmem, out_shape),
        compiler_params=pltpu.CompilerParams(vmem_limit_bytes=8 * 1024 * 1024),
    )(*places, *operands)


def virt_kernel(tiles_ref, place_ref, own_ref, other_ref, out_ref, whole_ref, part_ref, slot_ref):
    slot_count, half_rows, width = own_ref.shape
    own_count = part_ref.shape[0] // half_rows
    first = place_ref[0]
    half = place_ref[1]

    def note(s, carry):
        slot_ref[tiles_ref[s, 0] * NTV + tiles_ref[s, 1]] = s
        return carry

    lax.fori_loop(0, slot_count, note, 0)
    is_first = half == 0
    shape = (width, width)
    upper = lax.broadcasted_iota(jnp.int32, shape, 0) < lax.broadcasted_iota(jnp.int32, shape, 1)
    for r in range(NTV):
        for c in range(r, NTV):
            slot = slot_ref[r * NTV + c]
            mine = own_ref[slot]
            theirs = other_ref[slot]
            tile = jnp.concatenate(
                [jnp.where(is_first, mine, theirs), jnp.where(is_first, theirs, mine)], axis=0
            )
            if r == c:
                tile = jnp.where(upper, tile, jnp.zeros_like(tile))
            turned = tile.T
            if r == c:
                whole_ref[r, :, c * width : (c + 1) * width] = tile - turned
            else:
                whole_ref[r, :, c * width : (c + 1) * width] = tile
                whole_ref[c, :, r * width : (r + 1) * width] = -turned
    for i in range(own_count):
        left = whole_ref[tiles_ref[first + i, 0], pl.ds(half * half_rows, half_rows), :]
        right = whole_ref[tiles_ref[first + i, 1]]
        part_ref[i * half_rows : (i + 1) * half_rows] = lax.dot_general(
            left, right, (((1,), (1,)), ((), ())), preferred_element_type=jnp.float32
        )
    chunk = part_ref.shape[0] // out_ref.shape[0]
    for k in range(out_ref.shape[0]):
        out_ref[k] = message(part_ref[k * chunk : (k + 1) * chunk])


def virt_partial(tile_list, place, own, other, own_count, near):
    _, half_rows, width = own.shape
    rows = own_count * half_rows
    smem = pl.BlockSpec(memory_space=pltpu.SMEM)
    vmem = pl.BlockSpec(memory_space=pltpu.VMEM)
    return pl.pallas_call(
        virt_kernel,
        out_shape=jax.ShapeDtypeStruct((near, rows // near + GRAIN, width), jnp.int16),
        in_specs=[smem, smem, vmem, vmem],
        out_specs=vmem,
        scratch_shapes=[
            pltpu.VMEM((NTV, width, NTV * width), jnp.bfloat16),
            pltpu.VMEM((rows, width), jnp.float32),
            pltpu.SMEM((NTV * NTV,), jnp.int32),
        ],
        compiler_params=pltpu.CompilerParams(vmem_limit_bytes=24 * 1024 * 1024),
        name="virt_partial",
    )(tile_list, place, own, other)


def shards(amplitudes, pair_list, tile_list):
    _, slot_dev, row_dev, width = amplitudes.shape
    far = lax.axis_size("far")
    near = lax.axis_size("near")
    pair_count = far * near
    vir_at = lax.axis_index("vir")
    sub_at = lax.axis_index("sub")
    pair_at = lax.axis_index(("far", "near"))
    mine = amplitudes[0]
    share_rows = row_dev // pair_count
    share = mine.reshape(slot_dev, pair_count, share_rows, width)
    share = jnp.transpose(share, (1, 2, 0, 3)).reshape(pair_count, share_rows, slot_dev * width)
    got = lax.all_to_all(share, ("far", "near"), split_axis=0, concat_axis=0, tiled=True)
    own = lax.all_gather(mine, "vir", axis=0, tiled=True)
    other = lax.ppermute(own, "sub", [(0, 1), (1, 0)])
    place = jnp.stack([vir_at * slot_dev, sub_at, pair_at]).astype(jnp.int32)
    part = virt_partial(tile_list, place, own, other, slot_dev, near)
    own_list = lax.dynamic_slice_in_dim(tile_list, vir_at * slot_dev, slot_dev, 0)
    row = sub_at * row_dev + pair_at * share_rows + jnp.arange(share_rows, dtype=jnp.int32)
    column = jnp.arange(width, dtype=jnp.int32)
    lower = column[None, None, :] <= row[:, None, None]
    diagonal = (own_list[:, 0] == own_list[:, 1])[None, :, None]
    keep = jnp.logical_not(diagonal & lower).reshape(1, share_rows * slot_dev * width)
    rows = got.reshape(pair_count, share_rows * slot_dev * width)
    local_gram = lax.dot_general(
        jnp.where(keep, rows, jnp.zeros((), rows.dtype)),
        rows,
        (((1,), (1,)), ((), ())),
        preferred_element_type=jnp.float32,
    )
    blocks = width // pair_count
    packed_gram = local_gram.reshape(blocks, pair_count // blocks, pair_count)
    packed_gram = jnp.transpose(packed_gram, (1, 0, 2)).reshape(-1, width)
    chunk = slot_dev * row_dev // near
    near_parts = lax.all_to_all(part, "near", split_axis=0, concat_axis=0, tiled=True)
    gram_rows = lax.all_gather(packed_gram, "sub").sum(axis=0)
    gram_rows = lax.all_gather(gram_rows, "vir").sum(axis=0)
    long_rows = chunk + 3 * GRAIN
    far_block = in_vmem(
        near_kernel,
        jax.ShapeDtypeStruct((far, long_rows, width), jnp.int16),
        pair_list,
        near_parts,
        gram_rows,
        place=place,
    )
    far_parts = lax.all_to_all(far_block, "far", split_axis=0, concat_axis=0, tiled=True)
    last_block = in_vmem(
        far_kernel, jax.ShapeDtypeStruct((near, long_rows, width), jnp.int16), far_parts
    )
    spread = lax.all_to_all(last_block, "near", split_axis=0, concat_axis=0, tiled=True)
    virt_rows, p_occ = in_vmem(
        finish_kernel,
        (
            jax.ShapeDtypeStruct((near * chunk, width), jnp.float32),
            jax.ShapeDtypeStruct((OCC, OCC), jnp.float32),
        ),
        spread,
    )
    return (virt_rows.reshape(slot_dev, row_dev, width), p_occ)


def solution(mesh):
    groups, pair, vir, sub = (mesh.shape[name] for name in ("groups", "pair", "vir", "sub"))
    split = Mesh(
        mesh.devices.reshape(groups, pair // NEAR, NEAR, vir, sub),
        ("groups", "far", "near", "vir", "sub"),
    )
    in_specs = (
        P(("groups", "far", "near"), "vir", "sub", None),
        P(("groups", "far", "near"), None),
        P(),
    )
    out_specs = (P(("groups", "vir"), "sub", None), P("groups", None))
    return jax.shard_map(shards, mesh=split, in_specs=in_specs, out_specs=out_specs, check_vma=False)
```

```python
import jax
import jax.numpy as jnp
from jax import lax
from jax.experimental import pallas as pl
from jax.experimental.pallas import tpu as pltpu
from jax.sharding import Mesh
from jax.sharding import PartitionSpec as P


OCC = 256
NTV = 8
NEAR = 8
GRAIN = 8
STEPS = 256.0
TOP = 32767.0
FLOOR = 2.0**-120


def coded(values):
    largest = jnp.max(jnp.abs(values), axis=1, keepdims=True)
    k = jnp.floor(jnp.log2(jnp.maximum(largest, FLOOR)) * STEPS) + 2.0
    return (values * (jnp.exp2(k * (-1.0 / STEPS)) * TOP), k)


def rounded(values):
    return jnp.clip(jnp.floor(values + 0.5), -TOP, TOP)


def as_row(column, width):
    shape = (column.shape[0], width)
    here = lax.broadcasted_iota(jnp.int32, shape, 0) == lax.broadcasted_iota(jnp.int32, shape, 1)
    return jnp.sum(jnp.where(here, column, 0.0), axis=0, keepdims=True)


def as_column(row, count):
    shape = (count, row.shape[1])
    here = lax.broadcasted_iota(jnp.int32, shape, 0) == lax.broadcasted_iota(jnp.int32, shape, 1)
    return jnp.sum(jnp.where(here, row, 0.0), axis=1, keepdims=True)


def scale_of(row, count):
    return jnp.exp2(as_column(row, count) * (1.0 / STEPS)) * (1.0 / TOP)


def message(values, gram=None, ids=None):
    _, width = values.shape
    codes, k = coded(values)
    parts = [rounded(codes)]
    scales = [as_row(k, width)]
    if gram is not None:
        gram_codes, gram_k = coded(gram)
        high = rounded(gram_codes)
        parts += [high, rounded((gram_codes - high) * TOP)]
        scales += [as_row(gram_k, width), ids]
    spare = jnp.zeros((GRAIN - len(scales), width), jnp.float32)
    whole = jnp.concatenate([parts[0], jnp.concatenate([*scales, spare], axis=0), *parts[1:]], axis=0)
    return whole.astype(jnp.int32).astype(jnp.int16)


def opened(block, count, with_gram):
    words = block.astype(jnp.int32).astype(jnp.float32)
    values = words[:count] * scale_of(words[count : count + 1], count)
    if not with_gram:
        return (values, None, None)
    high = words[count + GRAIN : count + 2 * GRAIN]
    low = words[count + 2 * GRAIN : count + 3 * GRAIN]
    gram = (high + low * (1.0 / TOP)) * scale_of(words[count + 1 : count + 2], GRAIN)
    return (values, gram, words[count + 2 : count + 3])


def near_kernel(place_ref, pair_ref, parts_ref, gram_ref, out_ref):
    width = parts_ref.shape[2]
    pair_count = width // 4
    lane = lax.broadcasted_iota(jnp.int32, (1, width), 1)
    quarter = lane // pair_count
    swapped = (quarter == 1) | (quarter == 2)
    own_ids = jnp.where(swapped, pair_ref[:, 1:2], pair_ref[:, 0:1])
    ids = jnp.where(lane - quarter * pair_count == place_ref[2], own_ids, 0).astype(jnp.float32)
    count = parts_ref.shape[1] - GRAIN
    total, _, _ = opened(parts_ref[0], count, False)
    for k in range(1, parts_ref.shape[0]):
        total = total + opened(parts_ref[k], count, False)[0]
    block = message(total, gram_ref[...], ids)
    for k in range(out_ref.shape[0]):
        out_ref[k] = block


def far_kernel(parts_ref, out_ref):
    count = parts_ref.shape[1] - 3 * GRAIN
    total, gram, ids = opened(parts_ref[0], count, True)
    for k in range(1, parts_ref.shape[0]):
        more, more_gram, more_ids = opened(parts_ref[k], count, True)
        total = total + more
        gram = gram + more_gram
        ids = ids + more_ids
    block = message(total, gram, ids)
    for k in range(out_ref.shape[0]):
        out_ref[k] = block


def finish_kernel(spread_ref, virt_ref, occ_ref):
    near, _, width = spread_ref.shape
    chunk = virt_ref.shape[0] // near
    pair_count = width // 4
    packed, ids = 0.0, 0.0
    for k in range(near):
        values, gram, some_ids = opened(spread_ref[k], chunk, True)
        virt_ref[k * chunk : (k + 1) * chunk] = values
        packed = packed + gram
        ids = ids + some_ids
    gram = jnp.concatenate(
        [packed[:, k : k + pair_count] for k in range(0, width, pair_count)], axis=0
    )
    signed = jnp.concatenate(
        [jnp.concatenate([gram, -gram], axis=1), jnp.concatenate([-gram, gram], axis=1)], axis=0
    )
    orb_row = ids[:, : 2 * pair_count]
    partner_row = ids[:, 2 * pair_count :]
    orb_column = as_column(orb_row, 2 * pair_count)
    partner_column = as_column(partner_row, 2 * pair_count)
    couple = jnp.where(partner_column == partner_row, signed, 0.0)
    hot_shape = (2 * pair_count, OCC)
    across = lax.broadcasted_iota(jnp.int32, hot_shape, 1).astype(jnp.float32)
    down = lax.broadcasted_iota(jnp.int32, hot_shape[::-1], 0).astype(jnp.float32)
    hot = (orb_column == across).astype(jnp.float32)
    turned = (orb_row == down).astype(jnp.float32)
    inner = jnp.dot(couple, hot, precision=lax.Precision.HIGHEST)
    occ_ref[...] = -jnp.dot(turned, inner, precision=lax.Precision.HIGHEST)


def in_vmem(kernel, out_shape, *operands, place=None):
    vmem = pl.BlockSpec(memory_space=pltpu.VMEM)
    smem = pl.BlockSpec(memory_space=pltpu.SMEM)
    places = () if place is None else (place,)
    return pl.pallas_call(
        kernel,
        out_shape=out_shape,
        in_specs=[smem] * len(places) + [vmem] * len(operands),
        out_specs=jax.tree.map(lambda _: vmem, out_shape),
        compiler_params=pltpu.CompilerParams(vmem_limit_bytes=8 * 1024 * 1024),
    )(*places, *operands)


def virt_kernel(tiles_ref, place_ref, own_ref, other_ref, out_ref, whole_ref, part_ref, slot_ref):
    slot_count, half_rows, width = own_ref.shape
    own_count = part_ref.shape[0] // half_rows
    first = place_ref[0]
    half = place_ref[1]

    def note(s, carry):
        slot_ref[tiles_ref[s, 0] * NTV + tiles_ref[s, 1]] = s
        return carry

    lax.fori_loop(0, slot_count, note, 0)
    is_first = half == 0
    shape = (width, width)
    upper = lax.broadcasted_iota(jnp.int32, shape, 0) < lax.broadcasted_iota(jnp.int32, shape, 1)
    for r in range(NTV):
        for c in range(r, NTV):
            slot = slot_ref[r * NTV + c]
            mine = own_ref[slot]
            theirs = other_ref[slot]
            tile = jnp.concatenate(
                [jnp.where(is_first, mine, theirs), jnp.where(is_first, theirs, mine)], axis=0
            )
            if r == c:
                tile = jnp.where(upper, tile, jnp.zeros_like(tile))
            turned = tile.T
            if r == c:
                whole_ref[r, :, c * width : (c + 1) * width] = tile - turned
            else:
                whole_ref[r, :, c * width : (c + 1) * width] = tile
                whole_ref[c, :, r * width : (r + 1) * width] = -turned
    for i in range(own_count):
        left = whole_ref[tiles_ref[first + i, 0], pl.ds(half * half_rows, half_rows), :]
        right = whole_ref[tiles_ref[first + i, 1]]
        part_ref[i * half_rows : (i + 1) * half_rows] = lax.dot_general(
            left, right, (((1,), (1,)), ((), ())), preferred_element_type=jnp.float32
        )
    chunk = part_ref.shape[0] // out_ref.shape[0]
    for k in range(out_ref.shape[0]):
        out_ref[k] = message(part_ref[k * chunk : (k + 1) * chunk])


def virt_partial(tile_list, place, own, other, own_count, near):
    _, half_rows, width = own.shape
    rows = own_count * half_rows
    smem = pl.BlockSpec(memory_space=pltpu.SMEM)
    vmem = pl.BlockSpec(memory_space=pltpu.VMEM)
    return pl.pallas_call(
        virt_kernel,
        out_shape=jax.ShapeDtypeStruct((near, rows // near + GRAIN, width), jnp.int16),
        in_specs=[smem, smem, vmem, vmem],
        out_specs=vmem,
        scratch_shapes=[
            pltpu.VMEM((NTV, width, NTV * width), jnp.bfloat16),
            pltpu.VMEM((rows, width), jnp.float32),
            pltpu.SMEM((NTV * NTV,), jnp.int32),
        ],
        compiler_params=pltpu.CompilerParams(vmem_limit_bytes=24 * 1024 * 1024),
        name="virt_partial",
    )(tile_list, place, own, other)


def shards(amplitudes, pair_list, tile_list):
    _, slot_dev, row_dev, width = amplitudes.shape
    far = lax.axis_size("far")
    near = lax.axis_size("near")
    pair_count = far * near
    vir_at = lax.axis_index("vir")
    sub_at = lax.axis_index("sub")
    spot = lax.rem(lax.axis_index(("far", "near")) + pair_count // 2, pair_count)
    mine = amplitudes[0]
    share_rows = row_dev // pair_count
    share = mine.reshape(slot_dev, pair_count, share_rows, width)
    share = jnp.transpose(share, (1, 2, 0, 3)).reshape(pair_count, share_rows, slot_dev * width)
    order = [(k + pair_count // 2) % pair_count for k in range(pair_count)]
    got = lax.all_to_all(
        share,
        ("far", "near"),
        split_axis=0,
        concat_axis=0,
        axis_index_groups=[order],
        tiled=True,
    )
    own = lax.all_gather(mine, "vir", axis=0, tiled=True)
    other = lax.ppermute(own, "sub", [(0, 1), (1, 0)])
    place = jnp.stack([vir_at * slot_dev, sub_at, spot]).astype(jnp.int32)
    part = virt_partial(tile_list, place, own, other, slot_dev, near)
    own_list = lax.dynamic_slice_in_dim(tile_list, vir_at * slot_dev, slot_dev, 0)
    row = sub_at * row_dev + spot * share_rows + jnp.arange(share_rows, dtype=jnp.int32)
    column = jnp.arange(width, dtype=jnp.int32)
    lower = column[None, None, :] <= row[:, None, None]
    diagonal = (own_list[:, 0] == own_list[:, 1])[None, :, None]
    keep = jnp.logical_not(diagonal & lower).reshape(1, share_rows * slot_dev * width)
    rows = got.reshape(pair_count, share_rows * slot_dev * width)
    local_gram = lax.dot_general(
        jnp.where(keep, rows, jnp.zeros((), rows.dtype)),
        rows,
        (((1,), (1,)), ((), ())),
        preferred_element_type=jnp.float32,
    )
    blocks = width // pair_count
    packed_gram = local_gram.reshape(blocks, pair_count // blocks, pair_count)
    packed_gram = jnp.transpose(packed_gram, (1, 0, 2)).reshape(-1, width)
    chunk = slot_dev * row_dev // near
    near_parts = lax.all_to_all(part, "near", split_axis=0, concat_axis=0, tiled=True)
    gram_rows = lax.all_gather(packed_gram, "sub").sum(axis=0)
    gram_rows = lax.all_gather(gram_rows, "vir").sum(axis=0)
    long_rows = chunk + 3 * GRAIN
    far_block = in_vmem(
        near_kernel,
        jax.ShapeDtypeStruct((far, long_rows, width), jnp.int16),
        pair_list,
        near_parts,
        gram_rows,
        place=place,
    )
    far_parts = lax.all_to_all(far_block, "far", split_axis=0, concat_axis=0, tiled=True)
    last_block = in_vmem(
        far_kernel, jax.ShapeDtypeStruct((near, long_rows, width), jnp.int16), far_parts
    )
    spread = lax.all_to_all(last_block, "near", split_axis=0, concat_axis=0, tiled=True)
    virt_rows, p_occ = in_vmem(
        finish_kernel,
        (
            jax.ShapeDtypeStruct((near * chunk, width), jnp.float32),
            jax.ShapeDtypeStruct((OCC, OCC), jnp.float32),
        ),
        spread,
    )
    return (virt_rows.reshape(slot_dev, row_dev, width), p_occ)


def solution(mesh):
    groups, pair, vir, sub = (mesh.shape[name] for name in ("groups", "pair", "vir", "sub"))
    split = Mesh(
        mesh.devices.reshape(groups, pair // NEAR, NEAR, vir, sub),
        ("groups", "far", "near", "vir", "sub"),
    )
    in_specs = (
        P(("groups", "far", "near"), "vir", "sub", None),
        P(("groups", "far", "near"), None),
        P(),
    )
    out_specs = (P(("groups", "vir"), "sub", None), P("groups", None))
    return jax.shard_map(shards, mesh=split, in_specs=in_specs, out_specs=out_specs, check_vma=False)
```

```python
import jax
import jax.numpy as jnp
from jax import lax
from jax.experimental import pallas as pl
from jax.experimental.pallas import tpu as pltpu
from jax.sharding import Mesh
from jax.sharding import PartitionSpec as P


OCC = 256
NTV = 8
NEAR = 8
GRAIN = 8
STEPS = 256.0
TOP = 32767.0
FLOOR = 2.0**-120


def coded(values):
    largest = jnp.max(jnp.abs(values), axis=1, keepdims=True)
    k = jnp.floor(jnp.log2(jnp.maximum(largest, FLOOR)) * STEPS) + 2.0
    return (values * (jnp.exp2(k * (-1.0 / STEPS)) * TOP), k)


def rounded(values):
    return jnp.clip(jnp.floor(values + 0.5), -TOP, TOP)


def as_row(column, width):
    shape = (column.shape[0], width)
    here = lax.broadcasted_iota(jnp.int32, shape, 0) == lax.broadcasted_iota(jnp.int32, shape, 1)
    return jnp.sum(jnp.where(here, column, 0.0), axis=0, keepdims=True)


def as_column(row, count):
    shape = (count, row.shape[1])
    here = lax.broadcasted_iota(jnp.int32, shape, 0) == lax.broadcasted_iota(jnp.int32, shape, 1)
    return jnp.sum(jnp.where(here, row, 0.0), axis=1, keepdims=True)


def scale_of(row, count):
    return jnp.exp2(as_column(row, count) * (1.0 / STEPS)) * (1.0 / TOP)


def message(values, gram=None, ids=None):
    _, width = values.shape
    codes, k = coded(values)
    parts = [rounded(codes)]
    scales = [as_row(k, width)]
    if gram is not None:
        gram_codes, gram_k = coded(gram)
        high = rounded(gram_codes)
        parts += [high, rounded((gram_codes - high) * TOP)]
        scales += [as_row(gram_k, width), ids]
    spare = jnp.zeros((GRAIN - len(scales), width), jnp.float32)
    whole = jnp.concatenate([parts[0], jnp.concatenate([*scales, spare], axis=0), *parts[1:]], axis=0)
    return whole.astype(jnp.int32).astype(jnp.int16)


def opened(block, count, with_gram):
    words = block.astype(jnp.int32).astype(jnp.float32)
    values = words[:count] * scale_of(words[count : count + 1], count)
    if not with_gram:
        return (values, None, None)
    high = words[count + GRAIN : count + 2 * GRAIN]
    low = words[count + 2 * GRAIN : count + 3 * GRAIN]
    gram = (high + low * (1.0 / TOP)) * scale_of(words[count + 1 : count + 2], GRAIN)
    return (values, gram, words[count + 2 : count + 3])


def near_kernel(place_ref, pair_ref, parts_ref, gram_ref, out_ref):
    width = parts_ref.shape[2]
    pair_count = width // 4
    lane = lax.broadcasted_iota(jnp.int32, (1, width), 1)
    quarter = lane // pair_count
    swapped = (quarter == 1) | (quarter == 2)
    own_ids = jnp.where(swapped, pair_ref[:, 1:2], pair_ref[:, 0:1])
    ids = jnp.where(lane - quarter * pair_count == place_ref[2], own_ids, 0).astype(jnp.float32)
    count = parts_ref.shape[1] - GRAIN
    total, _, _ = opened(parts_ref[0], count, False)
    for k in range(1, parts_ref.shape[0]):
        total = total + opened(parts_ref[k], count, False)[0]
    block = message(total, gram_ref[...], ids)
    for k in range(out_ref.shape[0]):
        out_ref[k] = block


def far_kernel(parts_ref, out_ref):
    count = parts_ref.shape[1] - 3 * GRAIN
    total, gram, ids = opened(parts_ref[0], count, True)
    for k in range(1, parts_ref.shape[0]):
        more, more_gram, more_ids = opened(parts_ref[k], count, True)
        total = total + more
        gram = gram + more_gram
        ids = ids + more_ids
    block = message(total, gram, ids)
    for k in range(out_ref.shape[0]):
        out_ref[k] = block


def finish_kernel(spread_ref, virt_ref, occ_ref):
    near, _, width = spread_ref.shape
    chunk = virt_ref.shape[0] // near
    pair_count = width // 4
    packed, ids = 0.0, 0.0
    for k in range(near):
        values, gram, some_ids = opened(spread_ref[k], chunk, True)
        virt_ref[k * chunk : (k + 1) * chunk] = values
        packed = packed + gram
        ids = ids + some_ids
    gram = jnp.concatenate(
        [packed[:, k : k + pair_count] for k in range(0, width, pair_count)], axis=0
    )
    signed = jnp.concatenate(
        [jnp.concatenate([gram, -gram], axis=1), jnp.concatenate([-gram, gram], axis=1)], axis=0
    )
    orb_row = ids[:, : 2 * pair_count]
    partner_row = ids[:, 2 * pair_count :]
    orb_column = as_column(orb_row, 2 * pair_count)
    partner_column = as_column(partner_row, 2 * pair_count)
    couple = jnp.where(partner_column == partner_row, signed, 0.0)
    hot_shape = (2 * pair_count, OCC)
    across = lax.broadcasted_iota(jnp.int32, hot_shape, 1).astype(jnp.float32)
    down = lax.broadcasted_iota(jnp.int32, hot_shape[::-1], 0).astype(jnp.float32)
    hot = (orb_column == across).astype(jnp.float32)
    turned = (orb_row == down).astype(jnp.float32)
    inner = jnp.dot(couple, hot, precision=lax.Precision.HIGHEST)
    occ_ref[...] = -jnp.dot(turned, inner, precision=lax.Precision.HIGHEST)


def in_vmem(kernel, out_shape, *operands, place=None):
    vmem = pl.BlockSpec(memory_space=pltpu.VMEM)
    smem = pl.BlockSpec(memory_space=pltpu.SMEM)
    places = () if place is None else (place,)
    return pl.pallas_call(
        kernel,
        out_shape=out_shape,
        in_specs=[smem] * len(places) + [vmem] * len(operands),
        out_specs=jax.tree.map(lambda _: vmem, out_shape),
        compiler_params=pltpu.CompilerParams(vmem_limit_bytes=8 * 1024 * 1024),
    )(*places, *operands)


def virt_kernel(tiles_ref, place_ref, own_ref, other_ref, out_ref, whole_ref, part_ref, slot_ref):
    slot_count, half_rows, width = own_ref.shape
    own_count = part_ref.shape[0] // half_rows
    first = place_ref[0]
    half = place_ref[1]

    def note(s, carry):
        slot_ref[tiles_ref[s, 0] * NTV + tiles_ref[s, 1]] = s
        return carry

    lax.fori_loop(0, slot_count, note, 0)
    is_first = half == 0
    shape = (width, width)
    upper = lax.broadcasted_iota(jnp.int32, shape, 0) < lax.broadcasted_iota(jnp.int32, shape, 1)
    for r in range(NTV):
        for c in range(r, NTV):
            slot = slot_ref[r * NTV + c]
            mine = own_ref[slot]
            theirs = other_ref[slot]
            tile = jnp.concatenate(
                [jnp.where(is_first, mine, theirs), jnp.where(is_first, theirs, mine)], axis=0
            )
            if r == c:
                tile = jnp.where(upper, tile, jnp.zeros_like(tile))
            turned = tile.T
            if r == c:
                whole_ref[r, :, c * width : (c + 1) * width] = tile - turned
            else:
                whole_ref[r, :, c * width : (c + 1) * width] = tile
                whole_ref[c, :, r * width : (r + 1) * width] = -turned
    for i in range(own_count):
        left = whole_ref[tiles_ref[first + i, 0], pl.ds(half * half_rows, half_rows), :]
        right = whole_ref[tiles_ref[first + i, 1]]
        part_ref[i * half_rows : (i + 1) * half_rows] = lax.dot_general(
            left, right, (((1,), (1,)), ((), ())), preferred_element_type=jnp.float32
        )
    chunk = part_ref.shape[0] // out_ref.shape[0]
    for k in range(out_ref.shape[0]):
        out_ref[k] = message(part_ref[k * chunk : (k + 1) * chunk])


def virt_partial(tile_list, place, own, other, own_count, near):
    _, half_rows, width = own.shape
    rows = own_count * half_rows
    smem = pl.BlockSpec(memory_space=pltpu.SMEM)
    vmem = pl.BlockSpec(memory_space=pltpu.VMEM)
    return pl.pallas_call(
        virt_kernel,
        out_shape=jax.ShapeDtypeStruct((near, rows // near + GRAIN, width), jnp.int16),
        in_specs=[smem, smem, vmem, vmem],
        out_specs=vmem,
        scratch_shapes=[
            pltpu.VMEM((NTV, width, NTV * width), jnp.bfloat16),
            pltpu.VMEM((rows, width), jnp.float32),
            pltpu.SMEM((NTV * NTV,), jnp.int32),
        ],
        compiler_params=pltpu.CompilerParams(vmem_limit_bytes=24 * 1024 * 1024),
        name="virt_partial",
    )(tile_list, place, own, other)


def shards(amplitudes, pair_list, tile_list):
    _, slot_dev, row_dev, width = amplitudes.shape
    far = lax.axis_size("far")
    near = lax.axis_size("near")
    pair_count = far * near
    vir_at = lax.axis_index("vir")
    sub_at = lax.axis_index("sub")
    pair_at = lax.axis_index(("far", "near"))
    mine = amplitudes[0]
    share_rows = row_dev // pair_count
    share = mine.reshape(slot_dev, pair_count, share_rows, width)
    share = jnp.transpose(share, (1, 2, 0, 3)).reshape(pair_count, share_rows, slot_dev * width)
    got = lax.all_to_all(share, ("far", "near"), split_axis=0, concat_axis=0, tiled=True)
    own = lax.all_gather(mine, "vir", axis=0, tiled=True)
    other = lax.ppermute(own, "sub", [(0, 1), (1, 0)])
    place = jnp.stack([vir_at * slot_dev, sub_at, pair_at]).astype(jnp.int32)
    part = virt_partial(tile_list, place, own, other, slot_dev, near)
    own_list = lax.dynamic_slice_in_dim(tile_list, vir_at * slot_dev, slot_dev, 0)
    row = sub_at * row_dev + pair_at * share_rows + jnp.arange(share_rows, dtype=jnp.int32)
    column = jnp.arange(width, dtype=jnp.int32)
    lower = column[None, None, :] <= row[:, None, None]
    diagonal = (own_list[:, 0] == own_list[:, 1])[None, :, None]
    keep = jnp.logical_not(diagonal & lower).reshape(1, share_rows * slot_dev * width)
    rows = got.reshape(pair_count, share_rows * slot_dev * width)
    local_gram = lax.dot_general(
        jnp.where(keep, rows, jnp.zeros((), rows.dtype)),
        rows,
        (((1,), (1,)), ((), ())),
        preferred_element_type=jnp.float32,
    )
    blocks = width // pair_count
    packed_gram = local_gram.reshape(blocks, pair_count // blocks, pair_count)
    packed_gram = jnp.transpose(packed_gram, (1, 0, 2)).reshape(-1, width)
    chunk = slot_dev * row_dev // near
    near_parts = exchanged(part, "near", near // 2)
    gram_rows = lax.all_gather(packed_gram, "sub").sum(axis=0)
    gram_rows = lax.all_gather(gram_rows, "vir").sum(axis=0)
    long_rows = chunk + 3 * GRAIN
    far_block = in_vmem(
        near_kernel,
        jax.ShapeDtypeStruct((far, long_rows, width), jnp.int16),
        pair_list,
        near_parts,
        gram_rows,
        place=place,
    )
    far_parts = exchanged(far_block, "far", far // 2)
    last_block = in_vmem(
        far_kernel, jax.ShapeDtypeStruct((near, long_rows, width), jnp.int16), far_parts
    )
    spread = exchanged(last_block, "near", near // 2)
    virt_rows, p_occ = in_vmem(
        finish_kernel,
        (
            jax.ShapeDtypeStruct((near * chunk, width), jnp.float32),
            jax.ShapeDtypeStruct((OCC, OCC), jnp.float32),
        ),
        spread,
    )
    return (virt_rows.reshape(slot_dev, row_dev, width), p_occ)


def exchanged(array, axis, start):
    size = lax.axis_size(axis)
    order = [(start + k) % size for k in range(size)]
    return lax.all_to_all(
        array, axis, split_axis=0, concat_axis=0, axis_index_groups=[order], tiled=True
    )


def solution(mesh):
    groups, pair, vir, sub = (mesh.shape[name] for name in ("groups", "pair", "vir", "sub"))
    split = Mesh(
        mesh.devices.reshape(groups, pair // NEAR, NEAR, vir, sub),
        ("groups", "far", "near", "vir", "sub"),
    )
    in_specs = (
        P(("groups", "far", "near"), "vir", "sub", None),
        P(("groups", "far", "near"), None),
        P(),
    )
    out_specs = (P(("groups", "vir"), "sub", None), P("groups", None))
    return jax.shard_map(shards, mesh=split, in_specs=in_specs, out_specs=out_specs, check_vma=False)
```

```python
import jax
import jax.numpy as jnp
from jax import lax
from jax.experimental import pallas as pl
from jax.experimental.pallas import tpu as pltpu
from jax.sharding import Mesh
from jax.sharding import PartitionSpec as P


OCC = 256
NTV = 8
NEAR = 8
LEAD = 2
GRAIN = 8
STEPS = 256.0
TOP = 32767.0
FLOOR = 2.0**-120


def coded(values):
    largest = jnp.max(jnp.abs(values), axis=1, keepdims=True)
    k = jnp.floor(jnp.log2(jnp.maximum(largest, FLOOR)) * STEPS) + 2.0
    return (values * (jnp.exp2(k * (-1.0 / STEPS)) * TOP), k)


def rounded(values):
    return jnp.clip(jnp.floor(values + 0.5), -TOP, TOP)


def as_row(column, width):
    shape = (column.shape[0], width)
    here = lax.broadcasted_iota(jnp.int32, shape, 0) == lax.broadcasted_iota(jnp.int32, shape, 1)
    return jnp.sum(jnp.where(here, column, 0.0), axis=0, keepdims=True)


def as_column(row, count):
    shape = (count, row.shape[1])
    here = lax.broadcasted_iota(jnp.int32, shape, 0) == lax.broadcasted_iota(jnp.int32, shape, 1)
    return jnp.sum(jnp.where(here, row, 0.0), axis=1, keepdims=True)


def scale_of(row, count):
    return jnp.exp2(as_column(row, count) * (1.0 / STEPS)) * (1.0 / TOP)


def message(values, gram=None, ids=None):
    _, width = values.shape
    codes, k = coded(values)
    parts = [rounded(codes)]
    scales = [as_row(k, width)]
    if gram is not None:
        gram_codes, gram_k = coded(gram)
        high = rounded(gram_codes)
        parts += [high, rounded((gram_codes - high) * TOP)]
        scales += [as_row(gram_k, width), ids]
    spare = jnp.zeros((GRAIN - len(scales), width), jnp.float32)
    whole = jnp.concatenate([parts[0], jnp.concatenate([*scales, spare], axis=0), *parts[1:]], axis=0)
    return whole.astype(jnp.int32).astype(jnp.int16)


def opened(block, count, with_gram):
    words = block.astype(jnp.int32).astype(jnp.float32)
    values = words[:count] * scale_of(words[count : count + 1], count)
    if not with_gram:
        return (values, None, None)
    high = words[count + GRAIN : count + 2 * GRAIN]
    low = words[count + 2 * GRAIN : count + 3 * GRAIN]
    gram = (high + low * (1.0 / TOP)) * scale_of(words[count + 1 : count + 2], GRAIN)
    return (values, gram, words[count + 2 : count + 3])


def near_kernel(parts_ref, gram_ref, ids_ref, out_ref):
    count = parts_ref.shape[1] - GRAIN
    total, _, _ = opened(parts_ref[0], count, False)
    for k in range(1, parts_ref.shape[0]):
        total = total + opened(parts_ref[k], count, False)[0]
    block = message(total, gram_ref[...], ids_ref[...])
    for k in range(out_ref.shape[0]):
        out_ref[k] = block


def far_kernel(parts_ref, out_ref):
    count = parts_ref.shape[1] - 3 * GRAIN
    total, gram, ids = opened(parts_ref[0], count, True)
    for k in range(1, parts_ref.shape[0]):
        more, more_gram, more_ids = opened(parts_ref[k], count, True)
        total = total + more
        gram = gram + more_gram
        ids = ids + more_ids
    block = message(total, gram, ids)
    for k in range(out_ref.shape[0]):
        out_ref[k] = block


def finish_kernel(spread_ref, virt_ref, occ_ref):
    near, _, width = spread_ref.shape
    chunk = virt_ref.shape[0] // near
    pair_count = width // 4
    packed, ids = 0.0, 0.0
    for k in range(near):
        values, gram, some_ids = opened(spread_ref[k], chunk, True)
        virt_ref[k * chunk : (k + 1) * chunk] = values
        packed = packed + gram
        ids = ids + some_ids
    gram = jnp.concatenate(
        [packed[:, k : k + pair_count] for k in range(0, width, pair_count)], axis=0
    )
    signed = jnp.concatenate(
        [jnp.concatenate([gram, -gram], axis=1), jnp.concatenate([-gram, gram], axis=1)], axis=0
    )
    orb_row = ids[:, : 2 * pair_count]
    partner_row = ids[:, 2 * pair_count :]
    orb_column = as_column(orb_row, 2 * pair_count)
    partner_column = as_column(partner_row, 2 * pair_count)
    couple = jnp.where(partner_column == partner_row, signed, 0.0)
    hot_shape = (2 * pair_count, OCC)
    across = lax.broadcasted_iota(jnp.int32, hot_shape, 1).astype(jnp.float32)
    down = lax.broadcasted_iota(jnp.int32, hot_shape[::-1], 0).astype(jnp.float32)
    hot = (orb_column == across).astype(jnp.float32)
    turned = (orb_row == down).astype(jnp.float32)
    inner = jnp.dot(couple, hot, precision=lax.Precision.HIGHEST)
    occ_ref[...] = -jnp.dot(turned, inner, precision=lax.Precision.HIGHEST)


def in_vmem(kernel, out_shape, *operands):
    vmem = pl.BlockSpec(memory_space=pltpu.VMEM)
    return pl.pallas_call(
        kernel,
        out_shape=out_shape,
        in_specs=[vmem] * len(operands),
        out_specs=jax.tree.map(lambda _: vmem, out_shape),
        compiler_params=pltpu.CompilerParams(vmem_limit_bytes=8 * 1024 * 1024),
    )(*operands)


def virt_kernel(
    tiles_ref, place_ref, pair_ref, own_ref, other_ref, out_ref, ids_ref, whole_ref, part_ref, slot_ref
):
    slot_count, half_rows, width = own_ref.shape
    own_count = part_ref.shape[0] // half_rows
    first = place_ref[0]
    half = place_ref[1]

    def note(s, carry):
        slot_ref[tiles_ref[s, 0] * NTV + tiles_ref[s, 1]] = s
        return carry

    lax.fori_loop(0, slot_count, note, 0)
    is_first = half == 0
    shape = (width, width)
    upper = lax.broadcasted_iota(jnp.int32, shape, 0) < lax.broadcasted_iota(jnp.int32, shape, 1)
    for r in range(NTV):
        for c in range(r, NTV):
            slot = slot_ref[r * NTV + c]
            mine = own_ref[slot]
            theirs = other_ref[slot]
            tile = jnp.concatenate(
                [jnp.where(is_first, mine, theirs), jnp.where(is_first, theirs, mine)], axis=0
            )
            if r == c:
                tile = jnp.where(upper, tile, jnp.zeros_like(tile))
            turned = tile.T
            if r == c:
                whole_ref[r, :, c * width : (c + 1) * width] = tile - turned
            else:
                whole_ref[r, :, c * width : (c + 1) * width] = tile
                whole_ref[c, :, r * width : (r + 1) * width] = -turned
    for i in range(own_count):
        left = whole_ref[tiles_ref[first + i, 0], pl.ds(half * half_rows, half_rows), :]
        right = whole_ref[tiles_ref[first + i, 1]]
        part_ref[i * half_rows : (i + 1) * half_rows] = lax.dot_general(
            left, right, (((1,), (1,)), ((), ())), preferred_element_type=jnp.float32
        )
    chunk = part_ref.shape[0] // out_ref.shape[0]
    for k in range(out_ref.shape[0]):
        out_ref[k] = message(part_ref[k * chunk : (k + 1) * chunk])
    pair_count = width // 4
    lane = lax.broadcasted_iota(jnp.int32, (1, width), 1)
    quarter = lane // pair_count
    swapped = (quarter == 1) | (quarter == 2)
    own_ids = jnp.where(swapped, pair_ref[:, 1:2], pair_ref[:, 0:1])
    here = lane - quarter * pair_count == place_ref[2]
    ids_ref[...] = jnp.where(here, own_ids, 0).astype(jnp.float32)


def virt_partial(tile_list, place, pair_list, own, other, own_count, near):
    _, half_rows, width = own.shape
    rows = own_count * half_rows
    smem = pl.BlockSpec(memory_space=pltpu.SMEM)
    vmem = pl.BlockSpec(memory_space=pltpu.VMEM)
    return pl.pallas_call(
        virt_kernel,
        out_shape=(
            jax.ShapeDtypeStruct((near, rows // near + GRAIN, width), jnp.int16),
            jax.ShapeDtypeStruct((1, width), jnp.float32),
        ),
        in_specs=[smem, smem, vmem, vmem, vmem],
        out_specs=(vmem, vmem),
        scratch_shapes=[
            pltpu.VMEM((NTV, width, NTV * width), jnp.bfloat16),
            pltpu.VMEM((rows, width), jnp.float32),
            pltpu.SMEM((NTV * NTV,), jnp.int32),
        ],
        compiler_params=pltpu.CompilerParams(vmem_limit_bytes=24 * 1024 * 1024),
        name="virt_partial",
    )(tile_list, place, pair_list, own, other)


def shards(amplitudes, pair_list, tile_list):
    _, slot_dev, row_dev, width = amplitudes.shape
    far = lax.axis_size("far")
    near = lax.axis_size("near")
    pair_count = far * near
    vir_at = lax.axis_index("vir")
    sub_at = lax.axis_index("sub")
    pair_at = lax.rem(lax.axis_index(("far", "near")) + LEAD, pair_count)
    mine = amplitudes[0]
    share_rows = row_dev // pair_count
    share = mine.reshape(slot_dev, pair_count, share_rows, width)
    share = jnp.transpose(share, (1, 2, 0, 3)).reshape(pair_count, share_rows, slot_dev * width)
    order = [(k + pair_count - LEAD) % pair_count for k in range(pair_count)]
    got = lax.all_to_all(
        share,
        ("far", "near"),
        split_axis=0,
        concat_axis=0,
        axis_index_groups=[order],
        tiled=True,
    )
    own = lax.all_gather(mine, "vir", axis=0, tiled=True)
    other = lax.ppermute(own, "sub", [(0, 1), (1, 0)])
    place = jnp.stack([vir_at * slot_dev, sub_at, pair_at]).astype(jnp.int32)
    part, ids = virt_partial(tile_list, place, pair_list, own, other, slot_dev, near)
    own_list = lax.dynamic_slice_in_dim(tile_list, vir_at * slot_dev, slot_dev, 0)
    row = sub_at * row_dev + pair_at * share_rows + jnp.arange(share_rows, dtype=jnp.int32)
    column = jnp.arange(width, dtype=jnp.int32)
    lower = column[None, None, :] <= row[:, None, None]
    diagonal = (own_list[:, 0] == own_list[:, 1])[None, :, None]
    keep = jnp.logical_not(diagonal & lower).reshape(1, share_rows * slot_dev * width)
    rows = got.reshape(pair_count, share_rows * slot_dev * width)
    local_gram = lax.dot_general(
        jnp.where(keep, rows, jnp.zeros((), rows.dtype)),
        rows,
        (((1,), (1,)), ((), ())),
        preferred_element_type=jnp.float32,
    )
    blocks = width // pair_count
    packed_gram = local_gram.reshape(blocks, pair_count // blocks, pair_count)
    packed_gram = jnp.transpose(packed_gram, (1, 0, 2)).reshape(-1, width)
    chunk = slot_dev * row_dev // near
    near_parts = exchanged(part, "near", near // 2)
    gram_rows = lax.psum(packed_gram, ("vir", "sub"))
    long_rows = chunk + 3 * GRAIN
    far_block = in_vmem(
        near_kernel,
        jax.ShapeDtypeStruct((far, long_rows, width), jnp.int16),
        near_parts,
        gram_rows,
        ids,
    )
    far_parts = exchanged(far_block, "far", far // 2)
    last_block = in_vmem(
        far_kernel, jax.ShapeDtypeStruct((near, long_rows, width), jnp.int16), far_parts
    )
    spread = exchanged(last_block, "near", near // 2)
    virt_rows, p_occ = in_vmem(
        finish_kernel,
        (
            jax.ShapeDtypeStruct((near * chunk, width), jnp.float32),
            jax.ShapeDtypeStruct((OCC, OCC), jnp.float32),
        ),
        spread,
    )
    return (virt_rows.reshape(slot_dev, row_dev, width), p_occ)


def exchanged(array, axis, start):
    size = lax.axis_size(axis)
    order = [(start + k) % size for k in range(size)]
    return lax.all_to_all(
        array, axis, split_axis=0, concat_axis=0, axis_index_groups=[order], tiled=True
    )


def solution(mesh):
    groups, pair, vir, sub = (mesh.shape[name] for name in ("groups", "pair", "vir", "sub"))
    split = Mesh(
        mesh.devices.reshape(groups, pair // NEAR, NEAR, vir, sub),
        ("groups", "far", "near", "vir", "sub"),
    )
    in_specs = (
        P(("groups", "far", "near"), "vir", "sub", None),
        P(("groups", "far", "near"), None),
        P(),
    )
    out_specs = (P(("groups", "vir"), "sub", None), P("groups", None))
    return jax.shard_map(shards, mesh=split, in_specs=in_specs, out_specs=out_specs, check_vma=False)
```

```python
import jax
import jax.numpy as jnp
from jax import lax
from jax.experimental import pallas as pl
from jax.experimental.pallas import tpu as pltpu
from jax.sharding import Mesh
from jax.sharding import PartitionSpec as P


OCC = 256
NTV = 8
NEAR = 8
LEAD = 2
GRAIN = 8
STEPS = 256.0
TOP = 32767.0
FLOOR = 2.0**-120


def coded(values):
    largest = jnp.max(jnp.abs(values), axis=1, keepdims=True)
    k = jnp.floor(jnp.log2(jnp.maximum(largest, FLOOR)) * STEPS) + 2.0
    return (values * jnp.exp2(k * (-1.0 / STEPS)) * TOP, k)


def rounded(values):
    return jnp.clip(jnp.floor(values + 0.5), -TOP, TOP)


def as_row(column, width):
    shape = (column.shape[0], width)
    here = lax.broadcasted_iota(jnp.int32, shape, 0) == lax.broadcasted_iota(jnp.int32, shape, 1)
    return jnp.sum(jnp.where(here, column, 0.0), axis=0, keepdims=True)


def as_column(row, count):
    shape = (count, row.shape[1])
    here = lax.broadcasted_iota(jnp.int32, shape, 0) == lax.broadcasted_iota(jnp.int32, shape, 1)
    return jnp.sum(jnp.where(here, row, 0.0), axis=1, keepdims=True)


def scale_of(row, count):
    return jnp.exp2(as_column(row, count) * (1.0 / STEPS))


def message(values, gram=None, ids=None):
    _, width = values.shape
    codes, k = coded(values)
    parts = [rounded(codes)]
    scales = [as_row(k, width)]
    if gram is not None:
        gram_codes, gram_k = coded(gram)
        high = rounded(gram_codes)
        parts += [high, rounded((gram_codes - high) * TOP)]
        scales += [as_row(gram_k, width), ids]
    spare = jnp.zeros((GRAIN - len(scales), width), jnp.float32)
    whole = jnp.concatenate([parts[0], jnp.concatenate([*scales, spare], axis=0), *parts[1:]], axis=0)
    return whole.astype(jnp.int32).astype(jnp.int16)


def opened(block, count, with_gram):
    words = block.astype(jnp.int32).astype(jnp.float32)
    values = words[:count] * (1.0 / TOP) * scale_of(words[count : count + 1], count)
    if not with_gram:
        return (values, None, None)
    high = words[count + GRAIN : count + 2 * GRAIN]
    low = words[count + 2 * GRAIN : count + 3 * GRAIN]
    gram = (high + low * (1.0 / TOP)) * (1.0 / TOP) * scale_of(words[count + 1 : count + 2], GRAIN)
    return (values, gram, words[count + 2 : count + 3])


def near_kernel(parts_ref, gram_ref, ids_ref, out_ref):
    count = parts_ref.shape[1] - GRAIN
    total, _, _ = opened(parts_ref[0], count, False)
    for k in range(1, parts_ref.shape[0]):
        total = total + opened(parts_ref[k], count, False)[0]
    block = message(total, gram_ref[...], ids_ref[...])
    for k in range(out_ref.shape[0]):
        out_ref[k] = block


def far_kernel(parts_ref, out_ref):
    count = parts_ref.shape[1] - 3 * GRAIN
    total, gram, ids = opened(parts_ref[0], count, True)
    for k in range(1, parts_ref.shape[0]):
        more, more_gram, more_ids = opened(parts_ref[k], count, True)
        total = total + more
        gram = gram + more_gram
        ids = ids + more_ids
    block = message(total, gram, ids)
    for k in range(out_ref.shape[0]):
        out_ref[k] = block


def finish_kernel(spread_ref, virt_ref, occ_ref):
    near, _, width = spread_ref.shape
    chunk = virt_ref.shape[0] // near
    pair_count = width // 4
    packed, ids = 0.0, 0.0
    for k in range(near):
        values, gram, some_ids = opened(spread_ref[k], chunk, True)
        virt_ref[k * chunk : (k + 1) * chunk] = values
        packed = packed + gram
        ids = ids + some_ids
    gram = jnp.concatenate(
        [packed[:, k : k + pair_count] for k in range(0, width, pair_count)], axis=0
    )
    signed = jnp.concatenate(
        [jnp.concatenate([gram, -gram], axis=1), jnp.concatenate([-gram, gram], axis=1)], axis=0
    )
    orb_row = ids[:, : 2 * pair_count]
    partner_row = ids[:, 2 * pair_count :]
    orb_column = as_column(orb_row, 2 * pair_count)
    partner_column = as_column(partner_row, 2 * pair_count)
    couple = jnp.where(partner_column == partner_row, signed, 0.0)
    hot_shape = (2 * pair_count, OCC)
    across = lax.broadcasted_iota(jnp.int32, hot_shape, 1).astype(jnp.float32)
    down = lax.broadcasted_iota(jnp.int32, hot_shape[::-1], 0).astype(jnp.float32)
    hot = (orb_column == across).astype(jnp.float32)
    turned = (orb_row == down).astype(jnp.float32)
    inner = jnp.dot(couple, hot, precision=lax.Precision.HIGHEST)
    occ_ref[...] = -jnp.dot(turned, inner, precision=lax.Precision.HIGHEST)


def in_vmem(kernel, out_shape, *operands):
    vmem = pl.BlockSpec(memory_space=pltpu.VMEM)
    return pl.pallas_call(
        kernel,
        out_shape=out_shape,
        in_specs=[vmem] * len(operands),
        out_specs=jax.tree.map(lambda _: vmem, out_shape),
        compiler_params=pltpu.CompilerParams(vmem_limit_bytes=8 * 1024 * 1024),
    )(*operands)


def virt_kernel(
    tiles_ref, place_ref, pair_ref, own_ref, other_ref, out_ref, ids_ref, whole_ref, part_ref, slot_ref
):
    slot_count, half_rows, width = own_ref.shape
    own_count = part_ref.shape[0] // half_rows
    first = place_ref[0]
    half = place_ref[1]

    def note(s, carry):
        slot_ref[tiles_ref[s, 0] * NTV + tiles_ref[s, 1]] = s
        return carry

    lax.fori_loop(0, slot_count, note, 0)
    is_first = half == 0
    shape = (width, width)
    upper = lax.broadcasted_iota(jnp.int32, shape, 0) < lax.broadcasted_iota(jnp.int32, shape, 1)
    for r in range(NTV):
        for c in range(r, NTV):
            slot = slot_ref[r * NTV + c]
            mine = own_ref[slot]
            theirs = other_ref[slot]
            tile = jnp.concatenate(
                [jnp.where(is_first, mine, theirs), jnp.where(is_first, theirs, mine)], axis=0
            )
            if r == c:
                tile = jnp.where(upper, tile, jnp.zeros_like(tile))
            turned = tile.T
            if r == c:
                whole_ref[r, :, c * width : (c + 1) * width] = tile - turned
            else:
                whole_ref[r, :, c * width : (c + 1) * width] = tile
                whole_ref[c, :, r * width : (r + 1) * width] = -turned
    for i in range(own_count):
        left = whole_ref[tiles_ref[first + i, 0], pl.ds(half * half_rows, half_rows), :]
        right = whole_ref[tiles_ref[first + i, 1]]
        part_ref[i * half_rows : (i + 1) * half_rows] = lax.dot_general(
            left, right, (((1,), (1,)), ((), ())), preferred_element_type=jnp.float32
        )
    chunk = part_ref.shape[0] // out_ref.shape[0]
    for k in range(out_ref.shape[0]):
        out_ref[k] = message(part_ref[k * chunk : (k + 1) * chunk])
    pair_count = width // 4
    lane = lax.broadcasted_iota(jnp.int32, (1, width), 1)
    quarter = lane // pair_count
    swapped = (quarter == 1) | (quarter == 2)
    own_ids = jnp.where(swapped, pair_ref[:, 1:2], pair_ref[:, 0:1])
    here = lane - quarter * pair_count == place_ref[2]
    ids_ref[...] = jnp.where(here, own_ids, 0).astype(jnp.float32)


def virt_partial(tile_list, place, pair_list, own, other, own_count, near):
    _, half_rows, width = own.shape
    rows = own_count * half_rows
    smem = pl.BlockSpec(memory_space=pltpu.SMEM)
    vmem = pl.BlockSpec(memory_space=pltpu.VMEM)
    return pl.pallas_call(
        virt_kernel,
        out_shape=(
            jax.ShapeDtypeStruct((near, rows // near + GRAIN, width), jnp.int16),
            jax.ShapeDtypeStruct((1, width), jnp.float32),
        ),
        in_specs=[smem, smem, vmem, vmem, vmem],
        out_specs=(vmem, vmem),
        scratch_shapes=[
            pltpu.VMEM((NTV, width, NTV * width), jnp.bfloat16),
            pltpu.VMEM((rows, width), jnp.float32),
            pltpu.SMEM((NTV * NTV,), jnp.int32),
        ],
        compiler_params=pltpu.CompilerParams(vmem_limit_bytes=24 * 1024 * 1024),
        name="virt_partial",
    )(tile_list, place, pair_list, own, other)


def shards(amplitudes, pair_list, tile_list):
    _, slot_dev, row_dev, width = amplitudes.shape
    far = lax.axis_size("far")
    near = lax.axis_size("near")
    pair_count = far * near
    vir_at = lax.axis_index("vir")
    sub_at = lax.axis_index("sub")
    pair_at = lax.rem(lax.axis_index(("far", "near")) + LEAD, pair_count)
    mine = amplitudes[0]
    share_rows = row_dev // pair_count
    share = mine.reshape(slot_dev, pair_count, share_rows, width)
    share = jnp.transpose(share, (1, 0, 2, 3))
    order = [(k + pair_count - LEAD) % pair_count for k in range(pair_count)]
    got = lax.all_to_all(
        share,
        ("far", "near"),
        split_axis=0,
        concat_axis=0,
        axis_index_groups=[order],
        tiled=True,
    )
    own = lax.all_gather(mine, "vir", axis=0, tiled=True)
    other = lax.ppermute(own, "sub", [(0, 1), (1, 0)])
    place = jnp.stack([vir_at * slot_dev, sub_at, pair_at]).astype(jnp.int32)
    part, ids = virt_partial(tile_list, place, pair_list, own, other, slot_dev, near)
    own_list = lax.dynamic_slice_in_dim(tile_list, vir_at * slot_dev, slot_dev, 0)
    row = sub_at * row_dev + pair_at * share_rows + jnp.arange(share_rows, dtype=jnp.int32)
    column = jnp.arange(width, dtype=jnp.int32)
    lower = column[None, None, :] <= row[None, :, None]
    diagonal = (own_list[:, 0] == own_list[:, 1])[:, None, None]
    keep = jnp.logical_not(diagonal & lower).reshape(1, slot_dev * share_rows * width)
    rows = got.reshape(pair_count, share_rows * slot_dev * width)
    local_gram = lax.dot_general(
        jnp.where(keep, rows, jnp.zeros((), rows.dtype)),
        rows,
        (((1,), (1,)), ((), ())),
        preferred_element_type=jnp.float32,
    )
    blocks = width // pair_count
    packed_gram = local_gram.reshape(blocks, pair_count // blocks, pair_count)
    packed_gram = jnp.transpose(packed_gram, (1, 0, 2)).reshape(-1, width)
    chunk = slot_dev * row_dev // near
    near_parts = exchanged(part, "near", near // 2)
    gram_rows = lax.psum(packed_gram, ("vir", "sub"))
    long_rows = chunk + 3 * GRAIN
    far_block = in_vmem(
        near_kernel,
        jax.ShapeDtypeStruct((far, long_rows, width), jnp.int16),
        near_parts,
        gram_rows,
        ids,
    )
    far_parts = exchanged(far_block, "far", far // 2)
    last_block = in_vmem(
        far_kernel, jax.ShapeDtypeStruct((near, long_rows, width), jnp.int16), far_parts
    )
    spread = exchanged(last_block, "near", near // 2)
    virt_rows, p_occ = in_vmem(
        finish_kernel,
        (
            jax.ShapeDtypeStruct((near * chunk, width), jnp.float32),
            jax.ShapeDtypeStruct((OCC, OCC), jnp.float32),
        ),
        spread,
    )
    return (virt_rows.reshape(slot_dev, row_dev, width), p_occ)


def exchanged(array, axis, start):
    size = lax.axis_size(axis)
    order = [(start + k) % size for k in range(size)]
    return lax.all_to_all(
        array, axis, split_axis=0, concat_axis=0, axis_index_groups=[order], tiled=True
    )


def solution(mesh):
    groups, pair, vir, sub = (mesh.shape[name] for name in ("groups", "pair", "vir", "sub"))
    split = Mesh(
        mesh.devices.reshape(groups, pair // NEAR, NEAR, vir, sub),
        ("groups", "far", "near", "vir", "sub"),
    )
    in_specs = (
        P(("groups", "far", "near"), "vir", "sub", None),
        P(("groups", "far", "near"), None),
        P(),
    )
    out_specs = (P(("groups", "vir"), "sub", None), P("groups", None))
    return jax.shard_map(shards, mesh=split, in_specs=in_specs, out_specs=out_specs, check_vma=False)
```

```python
import jax
import jax.numpy as jnp
from jax import lax
from jax.experimental import pallas as pl
from jax.experimental.pallas import tpu as pltpu
from jax.sharding import Mesh
from jax.sharding import PartitionSpec as P


OCC = 256
NTV = 8
NEAR = 8
LEAD = 2
GRAIN = 8
STEPS = 256.0
TOP = 32767.0
FLOOR = 2.0**-120


def coded(values):
    largest = jnp.max(jnp.abs(values), axis=1, keepdims=True)
    k = jnp.floor(jnp.log2(jnp.maximum(largest, FLOOR)) * STEPS) + 2.0
    return (values * jnp.exp2(k * (-1.0 / STEPS)) * TOP, k)


def rounded(values):
    return jnp.clip(jnp.floor(values + 0.5), -TOP, TOP)


def as_row(column, width):
    shape = (column.shape[0], width)
    here = lax.broadcasted_iota(jnp.int32, shape, 0) == lax.broadcasted_iota(jnp.int32, shape, 1)
    return jnp.sum(jnp.where(here, column, 0.0), axis=0, keepdims=True)


def as_column(row, count):
    shape = (count, row.shape[1])
    here = lax.broadcasted_iota(jnp.int32, shape, 0) == lax.broadcasted_iota(jnp.int32, shape, 1)
    return jnp.sum(jnp.where(here, row, 0.0), axis=1, keepdims=True)


def scale_of(row, count):
    return jnp.exp2(as_column(row, count) * (1.0 / STEPS))


def message(values, gram=None, ids=None):
    _, width = values.shape
    codes, k = coded(values)
    parts = [rounded(codes)]
    scales = [as_row(k, width)]
    if gram is not None:
        gram_codes, gram_k = coded(gram)
        high = rounded(gram_codes)
        parts += [high, rounded((gram_codes - high) * TOP)]
        scales += [as_row(gram_k, width), ids]
    spare = jnp.zeros((GRAIN - len(scales), width), jnp.float32)
    whole = jnp.concatenate([parts[0], jnp.concatenate([*scales, spare], axis=0), *parts[1:]], axis=0)
    return whole.astype(jnp.int32).astype(jnp.int16)


def opened(block, count, with_gram):
    words = block.astype(jnp.int32).astype(jnp.float32)
    values = words[:count] * (1.0 / TOP) * scale_of(words[count : count + 1], count)
    if not with_gram:
        return (values, None, None)
    high = words[count + GRAIN : count + 2 * GRAIN]
    low = words[count + 2 * GRAIN : count + 3 * GRAIN]
    gram = (high + low * (1.0 / TOP)) * (1.0 / TOP) * scale_of(words[count + 1 : count + 2], GRAIN)
    return (values, gram, words[count + 2 : count + 3])


def near_kernel(parts_ref, gram_ref, ids_ref, out_ref):
    count = parts_ref.shape[1] - GRAIN
    total, _, _ = opened(parts_ref[0], count, False)
    for k in range(1, parts_ref.shape[0]):
        total = total + opened(parts_ref[k], count, False)[0]
    block = message(total, gram_ref[...], ids_ref[...])
    for k in range(out_ref.shape[0]):
        out_ref[k] = block


def far_kernel(parts_ref, out_ref):
    count = parts_ref.shape[1] - 3 * GRAIN
    total, gram, ids = opened(parts_ref[0], count, True)
    for k in range(1, parts_ref.shape[0]):
        more, more_gram, more_ids = opened(parts_ref[k], count, True)
        total = total + more
        gram = gram + more_gram
        ids = ids + more_ids
    block = message(total, gram, ids)
    for k in range(out_ref.shape[0]):
        out_ref[k] = block


def finish_kernel(spread_ref, virt_ref, gram_ref, ids_ref):
    near, _, _ = spread_ref.shape
    chunk = virt_ref.shape[0] // near
    packed, ids = 0.0, 0.0
    for k in range(near):
        values, gram, some_ids = opened(spread_ref[k], chunk, True)
        virt_ref[k * chunk : (k + 1) * chunk] = values
        packed = packed + gram
        ids = ids + some_ids
    gram_ref[...] = packed
    ids_ref[...] = ids


def occ_kernel(both_ref, ids_ref, occ_ref):
    packed = both_ref[0]
    for k in range(1, both_ref.shape[0]):
        packed = packed + both_ref[k]
    ids = ids_ref[...]
    width = ids.shape[1]
    pair_count = width // 4
    gram = jnp.concatenate(
        [packed[:, k : k + pair_count] for k in range(0, width, pair_count)], axis=0
    )
    signed = jnp.concatenate(
        [jnp.concatenate([gram, -gram], axis=1), jnp.concatenate([-gram, gram], axis=1)], axis=0
    )
    orb_row = ids[:, : 2 * pair_count]
    partner_row = ids[:, 2 * pair_count :]
    orb_column = as_column(orb_row, 2 * pair_count)
    partner_column = as_column(partner_row, 2 * pair_count)
    couple = jnp.where(partner_column == partner_row, signed, 0.0)
    hot_shape = (2 * pair_count, OCC)
    across = lax.broadcasted_iota(jnp.int32, hot_shape, 1).astype(jnp.float32)
    down = lax.broadcasted_iota(jnp.int32, hot_shape[::-1], 0).astype(jnp.float32)
    hot = (orb_column == across).astype(jnp.float32)
    turned = (orb_row == down).astype(jnp.float32)
    inner = jnp.dot(couple, hot, precision=lax.Precision.HIGHEST)
    occ_ref[...] = -jnp.dot(turned, inner, precision=lax.Precision.HIGHEST)


def in_vmem(kernel, out_shape, *operands):
    vmem = pl.BlockSpec(memory_space=pltpu.VMEM)
    return pl.pallas_call(
        kernel,
        out_shape=out_shape,
        in_specs=[vmem] * len(operands),
        out_specs=jax.tree.map(lambda _: vmem, out_shape),
        compiler_params=pltpu.CompilerParams(vmem_limit_bytes=8 * 1024 * 1024),
    )(*operands)


def virt_kernel(
    tiles_ref, place_ref, pair_ref, own_ref, other_ref, out_ref, ids_ref, whole_ref, part_ref, slot_ref
):
    slot_count, half_rows, width = own_ref.shape
    own_count = part_ref.shape[0] // half_rows
    first = place_ref[0]
    half = place_ref[1]

    def note(s, carry):
        slot_ref[tiles_ref[s, 0] * NTV + tiles_ref[s, 1]] = s
        return carry

    lax.fori_loop(0, slot_count, note, 0)
    is_first = half == 0
    shape = (width, width)
    upper = lax.broadcasted_iota(jnp.int32, shape, 0) < lax.broadcasted_iota(jnp.int32, shape, 1)
    for r in range(NTV):
        for c in range(r, NTV):
            slot = slot_ref[r * NTV + c]
            mine = own_ref[slot]
            theirs = other_ref[slot]
            tile = jnp.concatenate(
                [jnp.where(is_first, mine, theirs), jnp.where(is_first, theirs, mine)], axis=0
            )
            if r == c:
                tile = jnp.where(upper, tile, jnp.zeros_like(tile))
            turned = tile.T
            if r == c:
                whole_ref[r, :, c * width : (c + 1) * width] = tile - turned
            else:
                whole_ref[r, :, c * width : (c + 1) * width] = tile
                whole_ref[c, :, r * width : (r + 1) * width] = -turned
    for i in range(own_count):
        left = whole_ref[tiles_ref[first + i, 0], pl.ds(half * half_rows, half_rows), :]
        right = whole_ref[tiles_ref[first + i, 1]]
        part_ref[i * half_rows : (i + 1) * half_rows] = lax.dot_general(
            left, right, (((1,), (1,)), ((), ())), preferred_element_type=jnp.float32
        )
    chunk = part_ref.shape[0] // out_ref.shape[0]
    for k in range(out_ref.shape[0]):
        out_ref[k] = message(part_ref[k * chunk : (k + 1) * chunk])
    pair_count = width // 4
    lane = lax.broadcasted_iota(jnp.int32, (1, width), 1)
    quarter = lane // pair_count
    swapped = (quarter == 1) | (quarter == 2)
    own_ids = jnp.where(swapped, pair_ref[:, 1:2], pair_ref[:, 0:1])
    here = lane - quarter * pair_count == place_ref[2]
    ids_ref[...] = jnp.where(here, own_ids, 0).astype(jnp.float32)


def virt_partial(tile_list, place, pair_list, own, other, own_count, near):
    _, half_rows, width = own.shape
    rows = own_count * half_rows
    smem = pl.BlockSpec(memory_space=pltpu.SMEM)
    vmem = pl.BlockSpec(memory_space=pltpu.VMEM)
    return pl.pallas_call(
        virt_kernel,
        out_shape=(
            jax.ShapeDtypeStruct((near, rows // near + GRAIN, width), jnp.int16),
            jax.ShapeDtypeStruct((1, width), jnp.float32),
        ),
        in_specs=[smem, smem, vmem, vmem, vmem],
        out_specs=(vmem, vmem),
        scratch_shapes=[
            pltpu.VMEM((NTV, width, NTV * width), jnp.bfloat16),
            pltpu.VMEM((rows, width), jnp.float32),
            pltpu.SMEM((NTV * NTV,), jnp.int32),
        ],
        compiler_params=pltpu.CompilerParams(vmem_limit_bytes=24 * 1024 * 1024),
        name="virt_partial",
    )(tile_list, place, pair_list, own, other)


def shards(amplitudes, pair_list, tile_list):
    _, slot_dev, row_dev, width = amplitudes.shape
    far = lax.axis_size("far")
    near = lax.axis_size("near")
    pair_count = far * near
    vir_at = lax.axis_index("vir")
    sub_at = lax.axis_index("sub")
    pair_at = lax.rem(lax.axis_index(("far", "near")) + LEAD, pair_count)
    mine = amplitudes[0]
    share_rows = row_dev // pair_count
    share = mine.reshape(slot_dev, pair_count, share_rows, width)
    share = jnp.transpose(share, (1, 0, 2, 3))
    order = [(k + pair_count - LEAD) % pair_count for k in range(pair_count)]
    got = lax.all_to_all(
        share,
        ("far", "near"),
        split_axis=0,
        concat_axis=0,
        axis_index_groups=[order],
        tiled=True,
    )
    own = lax.all_gather(mine, "vir", axis=0, tiled=True)
    other = lax.ppermute(own, "sub", [(0, 1), (1, 0)])
    place = jnp.stack([vir_at * slot_dev, sub_at, pair_at]).astype(jnp.int32)
    part, ids = virt_partial(tile_list, place, pair_list, own, other, slot_dev, near)
    own_list = lax.dynamic_slice_in_dim(tile_list, vir_at * slot_dev, slot_dev, 0)
    row = sub_at * row_dev + pair_at * share_rows + jnp.arange(share_rows, dtype=jnp.int32)
    column = jnp.arange(width, dtype=jnp.int32)
    lower = column[None, None, :] <= row[None, :, None]
    diagonal = (own_list[:, 0] == own_list[:, 1])[:, None, None]
    keep = jnp.logical_not(diagonal & lower).reshape(1, slot_dev * share_rows * width)
    rows = got.reshape(pair_count, share_rows * slot_dev * width)
    local_gram = lax.dot_general(
        jnp.where(keep, rows, jnp.zeros((), rows.dtype)),
        rows,
        (((1,), (1,)), ((), ())),
        preferred_element_type=jnp.float32,
    )
    blocks = width // pair_count
    packed_gram = local_gram.reshape(blocks, pair_count // blocks, pair_count)
    packed_gram = jnp.transpose(packed_gram, (1, 0, 2)).reshape(-1, width)
    chunk = slot_dev * row_dev // near
    near_parts = exchanged(part, "near", near // 2)
    gram_rows = lax.psum(packed_gram, "vir")
    long_rows = chunk + 3 * GRAIN
    far_block = in_vmem(
        near_kernel,
        jax.ShapeDtypeStruct((far, long_rows, width), jnp.int16),
        near_parts,
        gram_rows,
        ids,
    )
    far_parts = exchanged(far_block, "far", far // 2)
    last_block = in_vmem(
        far_kernel, jax.ShapeDtypeStruct((near, long_rows, width), jnp.int16), far_parts
    )
    spread = exchanged(last_block, "near", near // 2)
    virt_rows, gram_part, all_ids = in_vmem(
        finish_kernel,
        (
            jax.ShapeDtypeStruct((near * chunk, width), jnp.float32),
            jax.ShapeDtypeStruct((GRAIN, width), jnp.float32),
            jax.ShapeDtypeStruct((1, width), jnp.float32),
        ),
        spread,
    )
    both = lax.all_gather(gram_part, "sub")
    p_occ = in_vmem(occ_kernel, jax.ShapeDtypeStruct((OCC, OCC), jnp.float32), both, all_ids)
    return (virt_rows.reshape(slot_dev, row_dev, width), p_occ)


def exchanged(array, axis, start):
    size = lax.axis_size(axis)
    order = [(start + k) % size for k in range(size)]
    return lax.all_to_all(
        array, axis, split_axis=0, concat_axis=0, axis_index_groups=[order], tiled=True
    )


def solution(mesh):
    groups, pair, vir, sub = (mesh.shape[name] for name in ("groups", "pair", "vir", "sub"))
    split = Mesh(
        mesh.devices.reshape(groups, pair // NEAR, NEAR, vir, sub),
        ("groups", "far", "near", "vir", "sub"),
    )
    in_specs = (
        P(("groups", "far", "near"), "vir", "sub", None),
        P(("groups", "far", "near"), None),
        P(),
    )
    out_specs = (P(("groups", "vir"), "sub", None), P("groups", None))
    return jax.shard_map(shards, mesh=split, in_specs=in_specs, out_specs=out_specs, check_vma=False)
```
